768 devices in a mesh: gx: 16 (over x, y_lo, core), gy: 48 (over y_hi, z).
Axes of the slice: x: 4, y: 8 (y_hi: 4, y_lo: 2; y = y_hi * 2 + y_lo), z: 12, core: 2. Of those that a mesh axis runs over, the one named last changes fastest.
Arguments:
- fields: float32 [5, 32, 128, 6144], P(None, None, 'gx', 'gy'), may hold values from -20 to 20, as said below
- coriolis: float32 [128], P('gx'), may hold values from 0.5 to 1.5
- slope_east: float32 [128, 6144], P('gx', 'gy'), may hold values from -3 to 3
- slope_north: float32 [128, 6144], P('gx', 'gy'), may hold values from -3 to 3
Outputs:
- updated: float32 [4, 32, 128, 6144], P(None, None, 'gx', 'gy')
The draws below stay inside these ranges and needn't reach their ends.
Inputs may be any that keep to these rules, and one draw needn't show every extreme that they name: `fields`: components in order: velocity along x, velocity along y, vertical velocity, potential temperature, pressure perturbation.
All inputs are finite; a program needn't handle non-finite values.
Results may differ from the reference program's by a relative error of at most 0.0003.
Values sent between devices are 32-bit elements; how exact they have to be, the bound alone decides.
A program may use at most 32 MiB of HBM per device.

```python
import jax
import jax.numpy as jnp
from jax import lax

NZ = 32
CY = 8
NX = 6144
NY = 128
N_GX = 16


def draw_fields(key, part):
    noise_key, amp_key = jax.random.split(key, 2)
    shape = (5, NZ, NY, NX)
    across = jnp.arange(NX, dtype=jnp.float32) / NX
    along = jnp.arange(NY, dtype=jnp.float32) / NY
    noise = jnp.clip(jax.random.normal(noise_key, shape, jnp.float32), -6.0, 6.0)
    ramp = 1.0 + along[:, None] + across[None, :]
    amplitude = jax.random.uniform(amp_key, (NZ,), jnp.float32, 0.5, 2.0)
    theta = noise[3] + amplitude[:, None, None] * ramp[None]
    return jnp.concatenate([noise[:3], theta[None], noise[4:]], axis=0)


def level_of(own_key, extent, shards, low, largest):
    level = 1.0
    for dim, blocks in shards:
        steps = jax.random.uniform(jax.random.fold_in(jax.random.fold_in(own_key, 6), dim), (blocks,), jnp.float32, low / len(shards), largest / len(shards))
        level = level * jnp.repeat(jnp.exp(steps), extent[dim] // blocks).reshape((-1,) + (1,) * (len(extent) - 1 - dim))
    return level


def gaussian(own_key, shape, scale, reach, cuts=(), kind=jnp.bfloat16):
    loudness = level_of(own_key, shape, cuts, -0.22, 0.18) if cuts else 1.0
    values = jax.random.normal(own_key, shape, jnp.float32) * scale * loudness
    return jnp.minimum(jnp.maximum(values, -reach), reach).astype(kind)


def setup_inputs(seed: int = 0) -> dict:
    keys = jax.random.split(jax.random.key(seed), 5)
    fields = draw_fields(jax.random.fold_in(keys[4], 71), 0)
    coriolis = jnp.clip(0.5 + 1.0 * jax.random.uniform(keys[1], (NY,), jnp.float32) ** level_of(keys[1], (NY,), ((0, 16),), -0.2, 0.2), 0.5, 1.5)
    slope_east = gaussian(keys[2], (NY, NX), 0.5, 3.0, ((0, 16), (1, 48)), jnp.float32)
    slope_north = gaussian(keys[3], (NY, NX), 0.5, 3.0, ((0, 16), (1, 48)), jnp.float32)
    return dict(fields=fields, coriolis=coriolis, slope_east=slope_east, slope_north=slope_north)


WENO_EPS = 1e-06
SECTION_DT = 0.3
SMAG_COEF = 0.06
BACKGROUND = 0.05
BUOYANCY = 0.5

def window(array, start, length, axis):
    return lax.slice_in_dim(array, start, start + length, axis=axis)

def weno_face(outer_low, inner_low, middle, inner_high, outer_high):
    smooth_zero = 13.0 / 12.0 * (outer_low - 2.0 * inner_low + middle) ** 2 + 0.25 * (outer_low - 4.0 * inner_low + 3.0 * middle) ** 2
    smooth_one = 13.0 / 12.0 * (inner_low - 2.0 * middle + inner_high) ** 2 + 0.25 * (inner_low - inner_high) ** 2
    smooth_two = 13.0 / 12.0 * (middle - 2.0 * inner_high + outer_high) ** 2 + 0.25 * (3.0 * middle - 4.0 * inner_high + outer_high) ** 2
    guess_zero = (2.0 * outer_low - 7.0 * inner_low + 11.0 * middle) / 6.0
    guess_one = (-inner_low + 5.0 * middle + 2.0 * inner_high) / 6.0
    guess_two = (2.0 * middle + 5.0 * inner_high - outer_high) / 6.0
    weight_zero = 0.1 / (WENO_EPS + smooth_zero) ** 2
    weight_one = 0.6 / (WENO_EPS + smooth_one) ** 2
    weight_two = 0.3 / (WENO_EPS + smooth_two) ** 2
    total = weight_zero + weight_one + weight_two
    return (weight_zero * guess_zero + weight_one * guess_one + weight_two * guess_two) / total

def faces_along(values, speed, axis, count):
    parts = [window(values, offset, count + 1, axis) for offset in range(6)]
    low_side = weno_face(parts[0], parts[1], parts[2], parts[3], parts[4])
    high_side = weno_face(parts[5], parts[4], parts[3], parts[2], parts[1])
    face_speed = (window(speed, 2, count + 1, axis) + window(speed, 3, count + 1, axis)) * 0.5
    return jnp.maximum(face_speed, 0.0) * low_side + jnp.minimum(face_speed, 0.0) * high_side

def divergence(flux, axis, count):
    return window(flux, 1, count, axis) - window(flux, 0, count, axis)

def section_update(extended, pressure, coriolis, slope_east, slope_north, theta_mean):
    depth = extended.shape[1]
    rows = extended.shape[2] - 6
    cols = extended.shape[3] - 6
    centre = extended[:, :, 3:-3, 3:-3]
    along_x = extended[:, :, 3:-3, :]
    flux_x = faces_along(along_x, along_x[0:1], 3, cols)
    along_y = extended[:, :, :, 3:-3]
    flux_y = faces_along(along_y, along_y[1:2], 2, rows)
    padded_z = jnp.pad(centre, ((0, 0), (3, 3), (0, 0), (0, 0)), mode='edge')
    flux_z = faces_along(padded_z, padded_z[2:3], 1, depth)
    face_index = lax.broadcasted_iota(jnp.int32, (1, depth + 1, 1, 1), 1)
    inside = jnp.logical_and(face_index > 0, face_index < depth).astype(flux_z.dtype)
    flux_z = flux_z * inside
    advection = -(divergence(flux_x, 3, cols) + divergence(flux_y, 2, rows) + divergence(flux_z, 1, depth))
    speed_x = extended[0]
    speed_y = extended[1]
    strain_xx = (speed_x[:, 2:-2, 3:-1] - speed_x[:, 2:-2, 1:-3]) * 0.5
    strain_yy = (speed_y[:, 3:-1, 2:-2] - speed_y[:, 1:-3, 2:-2]) * 0.5
    shear = (speed_x[:, 3:-1, 2:-2] - speed_x[:, 1:-3, 2:-2]) * 0.5 + (speed_y[:, 2:-2, 3:-1] - speed_y[:, 2:-2, 1:-3]) * 0.5
    eddy = SMAG_COEF * jnp.sqrt(2.0 * (strain_xx * strain_xx + strain_yy * strain_yy) + shear * shear + BACKGROUND)
    border = extended[:, :, 2:-2, 2:-2]
    eddy_x = (eddy[:, 1:-1, 1:] + eddy[:, 1:-1, :-1]) * 0.5
    diffuse_x = eddy_x * (border[:, :, 1:-1, 1:] - border[:, :, 1:-1, :-1])
    eddy_y = (eddy[:, 1:, 1:-1] + eddy[:, :-1, 1:-1]) * 0.5
    diffuse_y = eddy_y * (border[:, :, 1:, 1:-1] - border[:, :, :-1, 1:-1])
    mixing = diffuse_x[:, :, :, 1:] - diffuse_x[:, :, :, :-1] + diffuse_y[:, :, 1:, :] - diffuse_y[:, :, :-1, :]
    press_x = (pressure[:, 1:-1, 2:] - pressure[:, 1:-1, :-2]) * 0.5
    press_y = (pressure[:, 2:, 1:-1] - pressure[:, :-2, 1:-1]) * 0.5
    column = jnp.pad(pressure[:, 1:-1, 1:-1], ((1, 1), (0, 0), (0, 0)), mode='edge')
    press_z = (column[2:] - column[:-2]) * 0.5
    level_index = lax.broadcasted_iota(jnp.int32, (depth, 1, 1), 0).astype(centre.dtype)
    level_factor = 1.0 - (level_index + 0.5) / depth
    turning = coriolis[None, :, None]
    force_u = -(press_x - slope_east[None] * level_factor * press_z) + turning * centre[1]
    force_v = -(press_y - slope_north[None] * level_factor * press_z) - turning * centre[0]
    force_w = -press_z + BUOYANCY * (centre[3] - theta_mean[:, None, None])
    forcing = jnp.stack([force_u, force_v, force_w, jnp.zeros_like(force_w)])
    return centre + SECTION_DT * (advection + mixing + forcing)

def reference(fields, coriolis, slope_east, slope_north):
    theta_mean = lax.optimization_barrier(jnp.sum(fields[3], axis=(1, 2))) / (NX * NY)
    padded = jnp.pad(fields, ((0, 0), (0, 0), (3, 3), (3, 3)))

    def one_block(block):
        start = (block * CY).astype(jnp.int32)
        piece = lax.dynamic_slice_in_dim(padded, start, CY + 6, 2)
        turning = lax.dynamic_slice_in_dim(coriolis, start, CY, 0)
        east = lax.dynamic_slice_in_dim(slope_east, start, CY, 0)
        north = lax.dynamic_slice_in_dim(slope_north, start, CY, 0)
        return section_update(piece[:4], piece[4, :, 2:-2, 2:-2], turning, east, north, theta_mean)
    blocks = lax.map(one_block, jnp.arange(N_GX, dtype=jnp.int32))
    return jnp.transpose(blocks, (1, 2, 0, 3, 4)).reshape(4, NZ, NY, NX)
```

```python
import functools

import jax
import jax.numpy as jnp
from jax import lax
from jax.experimental import pallas as pl
from jax.experimental.pallas import tpu as pltpu
from jax.sharding import Mesh
from jax.sharding import PartitionSpec as P

AXES = ("gx_0", "gx_1", "gx_2", "gy_0", "gy_1")
GX = ("gx_0", "gx_1", "gx_2")
GY = ("gy_0", "gy_1")
MESH = pl.DeviceIdType.MESH

WENO_EPS = 1e-06
SECTION_DT = 0.3
SMAG_COEF = 0.06
BACKGROUND = 0.05
BUOYANCY = 0.5

LANES = 128
ROWS = 8
EDGE = 24


def line_terms(q, sigma, size, upward, mixing):
    count = len(q) - 6
    g = [q[i + 1] - q[i] for i in range(count + 5)]
    bend = [g[i + 1] - g[i] for i in range(count + 4)]
    third = [bend[i + 1] - bend[i] for i in range(count + 3)]
    mid, low, high = [], [], []
    for i in range(count + 4):
        before, after, d = g[i], g[i + 1], bend[i]
        a = (d * (4.0 / 3.0)) * d + (before * after + WENO_EPS)
        d2 = d + d
        b = a + after * d2
        c = a - before * d2
        mid.append(a * a)
        low.append(b * b)
        high.append(c * c)
    out = []
    for f in range(count + 1):
        up = upward[f]
        e0 = jnp.where(up, low[f], high[f + 3])
        e1 = jnp.where(up, mid[f + 1], mid[f + 2])
        e2 = jnp.where(up, high[f + 2], low[f + 1])
        curve = jnp.where(up, bend[f + 1], bend[f + 2])
        t0 = jnp.where(up, third[f], third[f + 2])
        u = e0 * 3.0
        v = e2 + e2
        den = e1 * (e2 + u) + u * v
        num = e1 * (u * third[f + 1] + v * t0)
        flux = sigma[f] * ((q[f + 2] + q[f + 3]) - curve * (1.0 / 3.0)) + size[f] * (num / den)
        if mixing is not None:
            flux = flux + mixing[f] * g[f + 2]
        out.append(flux)
    return out


def speeds(s, keep_first=None, keep_last=None):
    count = len(s) - 6
    sigma = [(s[f + 2] + s[f + 3]) * (-0.25 * SECTION_DT) for f in range(count + 1)]
    if keep_first is not None:
        sigma[0] = jnp.where(keep_first, sigma[0], 0.0)
        sigma[count] = jnp.where(keep_last, sigma[count], 0.0)
    upward = [x < 0.0 for x in sigma]
    size = [jnp.abs(x) * (1.0 / 3.0) for x in sigma]
    return sigma, size, upward


def kernel(
    sizes, fields, coriolis, slope_east, slope_north, out,
    zf, xt, ysend, yrecv, halo, csend, crecv, eddy_y, eddy_z, eddy_v, eddy_x, xdiv, east, north, cor,
    row_send, recv_a, recv_z, recv_y,
    load_sem, send_a, got_a, send_z, got_z, send_y, got_y, send_h, got_h,
):
    nx, nl, nc, nh, nz = sizes
    ny = nh * nl
    n_gx, n_gy = nx * nl * nc, nh * nz
    depth = out.shape[1] // ROWS
    groups = depth // ROWS
    px, pl_, pc, ph, pz = (lax.axis_index(a) for a in AXES)
    py = ph * nl + pl_
    gx = (px * nl + pl_) * nc + pc
    gy = ph * nz + pz

    def at_gx(i):
        i = lax.rem(i + n_gx, n_gx)
        return (i // (nl * nc), lax.rem(i // nc, nl), lax.rem(i, nc), ph, pz)

    def at_gy(i):
        i = lax.rem(i + n_gy, n_gy)
        return (px, pl_, pc, i // nz, lax.rem(i, nz))

    peers_a = [
        (lax.rem(px + dx, nx), pl_, lax.rem(pc + dc, nc), ph, pz)
        for dx in range(nx)
        for dc in range(nc)
        if dx or dc
    ]
    peers_z = [(px, pl_, pc, ph, lax.rem(pz + dz, nz)) for dz in range(1, nz)]
    peers_y = []
    for dy in range(1, ny):
        y = lax.rem(py + dy, ny)
        peers_y.append((px, lax.rem(y, nl), pc, y // nl, pz))
    gx_low, gx_high = at_gx(gx - 1), at_gx(gx + 1)
    gy_low, gy_high = at_gy(gy - 1), at_gy(gy + 1)

    main = pl.ds(EDGE, depth * ROWS)
    loads = [
        pltpu.make_async_copy(fields.at[f], zf.at[f, main], load_sem.at[f]) for f in (3, 0, 1, 2, 4)
    ]
    loads.append(pltpu.make_async_copy(slope_east, east, load_sem.at[5]))
    loads.append(pltpu.make_async_copy(slope_north, north, load_sem.at[6]))
    loads.append(pltpu.make_async_copy(coriolis, cor, load_sem.at[7]))
    for copy in loads:
        copy.start()

    barrier = pltpu.get_barrier_semaphore()
    everyone = [*peers_a, *peers_z, *peers_y, gx_low, gx_high, gy_low, gy_high]
    for peer in everyone:
        pl.semaphore_signal(barrier, inc=1, device_id=peer, device_id_type=MESH)

    lane = lax.broadcasted_iota(jnp.int32, (ROWS, LANES), 1)
    sub = lax.broadcasted_iota(jnp.int32, (ROWS, LANES), 0)

    def strided(ref, f, first):
        return ref[f, pl.ds(first, ROWS, stride=ROWS), :]

    loads[0].wait()
    own = jnp.zeros((ROWS, LANES), jnp.float32)
    for g in range(groups):
        level = strided(zf, 3, EDGE + 64 * g)
        for j in range(1, ROWS):
            level = level + strided(zf, 3, EDGE + 64 * g + j)
        own = own + jnp.where(lane == sub + ROWS * g, jnp.sum(level, axis=1, keepdims=True), 0.0)
    own = jnp.sum(own, axis=0, keepdims=True)
    row_send[0] = own

    def remote(src, dst, send, got, peer):
        return pltpu.make_async_remote_copy(
            src_ref=src, dst_ref=dst, send_sem=send, recv_sem=got, device_id=peer, device_id_type=MESH
        )

    def phase(index, peers, dst, send, got):
        copies = [
            remote(row_send.at[index], dst.at[i], send.at[i], got.at[i], peer)
            for i, peer in enumerate(peers)
        ]
        for copy in copies:
            copy.start()
        return copies

    def total_of(copies, dst, value):
        for i, copy in enumerate(copies):
            copy.wait_recv()
        for i in range(len(copies)):
            value = value + dst[i]
        return value

    pl.semaphore_wait(barrier, len(everyone))
    first = phase(0, peers_a, recv_a, send_a, got_a)

    for copy in loads[1:]:
        copy.wait()

    for f in range(5):
        for r in range(3):
            slab = r * 4 + f
            if f == 4:
                if r:
                    continue
                slab = 12
            low_row, high_row = (r, 5 + r) if f < 4 else (0, 7)
            ysend[0, slab] = zf[f, pl.ds(EDGE + low_row, depth, stride=ROWS), :]
            ysend[1, slab] = zf[f, pl.ds(EDGE + high_row, depth, stride=ROWS), :]
        bottom = zf[f, pl.ds(EDGE, ROWS), :]
        top = zf[f, pl.ds(EDGE + (depth - 1) * ROWS, ROWS), :]
        for r in range(3):
            zf[f, pl.ds(r * ROWS, ROWS), :] = bottom
            zf[f, pl.ds(EDGE + (depth + r) * ROWS, ROWS), :] = top
    halves = depth * ROWS // LANES

    def turn(i, carry):
        f, half = i // halves, lax.rem(i, halves)
        block = zf[f, pl.ds(EDGE + half * LANES, LANES), :]
        xt[f, half, pl.ds(ROWS, LANES), :] = block.T
        return carry

    lax.fori_loop(0, 5 * halves, turn, 0)

    y_copies = [
        remote(ysend.at[0], yrecv.at[1], send_h.at[0], got_h.at[0], gx_low),
        remote(ysend.at[1], yrecv.at[0], send_h.at[1], got_h.at[1], gx_high),
    ]
    for copy in y_copies:
        copy.start()

    turning = jnp.zeros((ROWS, LANES), jnp.float32)
    for j in range(ROWS):
        turning = jnp.where(sub == j, cor[j] * SECTION_DT, turning)

    def upright(c, carry):
        base = c * ROWS * ROWS

        def cells(f, first=0, count=ROWS + 6):
            return [zf[f, pl.ds(base + (first + i) * ROWS, ROWS), :] for i in range(count)]

        p = cells(4, 2, ROWS + 2)
        slope = [(p[i + 2] - p[i]) * (0.5 * SECTION_DT) for i in range(ROWS)]
        top_factor = 1.0 - (c * ROWS).astype(jnp.float32) / depth
        w = cells(2)
        sigma, size, upward = speeds(w, c > 0, c < groups - 1)
        for f in range(4):
            q = w if f == 2 else cells(f)
            flux = line_terms(q, sigma, size, upward, None)
            for i in range(ROWS):
                value = q[i + 3] + (flux[i + 1] - flux[i])
                rows = pl.ds(base + i * ROWS, ROWS)
                if f == 0:
                    tilt = slope[i] * (top_factor - (i + 0.5) / depth)
                    value = value + east[...] * tilt + turning * zf[1, pl.ds(base + EDGE + i * ROWS, ROWS), :]
                elif f == 1:
                    tilt = slope[i] * (top_factor - (i + 0.5) / depth)
                    value = value + north[...] * tilt - turning * zf[0, pl.ds(base + EDGE + i * ROWS, ROWS), :]
                elif f == 2:
                    warm = zf[3, pl.ds(base + EDGE + i * ROWS, ROWS), :]
                    value = value - slope[i] + warm * (SECTION_DT * BUOYANCY)
                out[f, rows, :] = value
        return carry

    lax.fori_loop(0, groups, upright, 0)

    own = total_of(first, recv_a, own)
    row_send[1] = own
    x_copies = [
        remote(xt.at[:, :, pl.ds(ROWS, ROWS)], xt.at[:, :, pl.ds(ROWS + LANES, ROWS)], send_h.at[2], got_h.at[2], gy_low),
        remote(xt.at[:, :, pl.ds(LANES, ROWS)], xt.at[:, :, pl.ds(0, ROWS)], send_h.at[3], got_h.at[3], gy_high),
    ]
    second = phase(1, peers_z, recv_z, send_z, got_z)
    for copy in x_copies:
        copy.start()
    for copy in x_copies:
        copy.wait_recv()

    edge_rows = jnp.zeros((5, halves, ROWS, LANES), jnp.float32)

    @pl.when(gy == 0)
    def _():
        xt[:, :, pl.ds(0, ROWS), :] = edge_rows

    @pl.when(gy == n_gy - 1)
    def _():
        xt[:, :, pl.ds(ROWS + LANES, ROWS), :] = edge_rows

    gap = jnp.zeros((LANES - 2 * ROWS, LANES), jnp.float32)
    for f in range(2):
        for half in range(halves):
            block = jnp.concatenate(
                [xt[f, half, pl.ds(ROWS + LANES, ROWS), :], gap, xt[f, half, pl.ds(0, ROWS), :]], axis=0
            )
            halo[f, pl.ds(half * LANES, LANES), :] = block.T
    for f in range(2):
        csend[0, f] = halo[f, pl.ds(0, depth, stride=ROWS), :]
        csend[1, f] = halo[f, pl.ds(7, depth, stride=ROWS), :]

    own = total_of(second, recv_z, own)
    row_send[2] = own
    third = phase(2, peers_y, recv_y, send_y, got_y)
    c_copies = [
        remote(csend.at[0], crecv.at[1], send_h.at[4], got_h.at[4], gx_low),
        remote(csend.at[1], crecv.at[0], send_h.at[5], got_h.at[5], gx_high),
    ]
    for copy in c_copies:
        copy.start()
    for copy in y_copies + c_copies:
        copy.wait_recv()

    for side, at_edge in ((0, gx == 0), (1, gx == n_gx - 1)):

        @pl.when(at_edge)
        def _():
            yrecv[side] = jnp.zeros(yrecv.shape[1:], jnp.float32)
            crecv[side] = jnp.zeros(crecv.shape[1:], jnp.float32)

    def row(f, j, g):
        if j < 0:
            return yrecv[0, (j + 3) * 4 + f if f < 4 else 12, pl.ds(g * ROWS, ROWS), :]
        if j >= ROWS:
            return yrecv[1, (j - ROWS) * 4 + f if f < 4 else 12, pl.ds(g * ROWS, ROWS), :]
        return strided(zf, f, EDGE + g * 64 + j)

    def halo_row(f, j, g):
        if j < 0:
            return crecv[0, f, pl.ds(g * ROWS, ROWS), :]
        if j >= ROWS:
            return crecv[1, f, pl.ds(g * ROWS, ROWS), :]
        return strided(halo, f, g * 64 + j)

    def strength(ux, vx, uy, vy):
        cross = uy + vx
        return SMAG_COEF * jnp.sqrt(0.5 * (ux * ux + vy * vy) + 0.25 * (cross * cross) + BACKGROUND)

    def eddies(g, carry):
        u = [row(0, j, g) for j in range(-2, ROWS + 2)]
        v = [row(1, j, g) for j in range(-2, ROWS + 2)]
        hu = [halo_row(0, j, g) for j in range(-1, ROWS + 1)]
        hv = [halo_row(1, j, g) for j in range(-1, ROWS + 1)]
        left, right = lane == LANES - 1, lane == 0

        def across(inner, outer):
            plus = pltpu.roll(jnp.where(right, outer, inner), LANES - 1, 1)
            minus = pltpu.roll(jnp.where(left, outer, inner), 1, 1)
            return plus - minus

        for j in range(-1, ROWS + 1):
            ux, vx = across(u[j + 2], hu[j + 1]), across(v[j + 2], hv[j + 1])
            uy, vy = u[j + 3] - u[j + 1], v[j + 3] - v[j + 1]
            e = strength(ux, vx, uy, vy)
            eddy_y[j + 1, pl.ds(g * ROWS, ROWS), :] = e
            if 0 <= j < ROWS:
                eddy_z[pl.ds(g * 64 + j, ROWS, stride=ROWS), :] = e
                ux, vx = across(hu[j + 1], u[j + 2]), across(hv[j + 1], v[j + 2])
                uy, vy = hu[j + 2] - hu[j], hv[j + 2] - hv[j]
                eddy_v[pl.ds(g * 64 + j, ROWS, stride=ROWS), :] = strength(ux, vx, uy, vy)
        return carry

    lax.fori_loop(0, groups, eddies, 0)
    for half in range(halves):
        eddy_x[half, pl.ds(ROWS, LANES), :] = eddy_z[pl.ds(half * LANES, LANES), :].T
        outer = eddy_v[pl.ds(half * LANES, LANES), :].T
        eddy_x[half, pl.ds(0, ROWS), :] = outer[LANES - ROWS :]
        eddy_x[half, pl.ds(ROWS + LANES, ROWS), :] = outer[:ROWS]

    def northward(g, carry):
        v = [row(1, j, g) for j in range(-3, ROWS + 3)]
        sigma, size, upward = speeds(v)
        e = [eddy_y[j, pl.ds(g * ROWS, ROWS), :] for j in range(ROWS + 2)]
        mixing = [(e[f] + e[f + 1]) * (0.5 * SECTION_DT) for f in range(ROWS + 1)]
        p = [row(4, j, g) for j in range(-1, ROWS + 1)]
        for f in range(4):
            q = v if f == 1 else [row(f, j, g) for j in range(-3, ROWS + 3)]
            flux = line_terms(q, sigma, size, upward, mixing)
            for j in range(ROWS):
                value = flux[j + 1] - flux[j]
                if f == 1:
                    value = value - (p[j + 2] - p[j]) * (0.5 * SECTION_DT)
                rows = pl.ds(g * 64 + j, ROWS, stride=ROWS)
                out[f, rows, :] = out[f, rows, :] + value
        return carry

    lax.fori_loop(0, groups, northward, 0)

    step = LANES // ROWS

    def eastward(c, carry):
        half, start = c // 2, lax.rem(c, 2) * ROWS

        def cells(f, first=-3, count=ROWS + 6):
            return [
                xt[f, half, pl.ds(start + (ROWS + first + i), ROWS, stride=step), :] for i in range(count)
            ]

        u = cells(0)
        sigma, size, upward = speeds(u)
        e = [eddy_x[half, pl.ds(start + (ROWS - 1 + i), ROWS, stride=step), :] for i in range(ROWS + 2)]
        mixing = [(e[f] + e[f + 1]) * (0.5 * SECTION_DT) for f in range(ROWS + 1)]
        p = cells(4, -1, ROWS + 2)
        for f in range(4):
            q = u if f == 0 else cells(f)
            flux = line_terms(q, sigma, size, upward, mixing)
            for i in range(ROWS):
                value = flux[i + 1] - flux[i]
                if f == 0:
                    value = value - (p[i + 2] - p[i]) * (0.5 * SECTION_DT)
                xdiv[f, half, pl.ds(start + i, ROWS, stride=step), :] = value
        return carry

    lax.fori_loop(0, 2 * halves, eastward, 0)

    def turn_back(i, carry):
        f, half = i // halves, lax.rem(i, halves)
        rows = pl.ds(half * LANES, LANES)
        out[f, rows, :] = out[f, rows, :] + xdiv[f, half].T
        return carry

    lax.fori_loop(0, 4 * halves, turn_back, 0)

    own = total_of(third, recv_y, own)
    scale = SECTION_DT * BUOYANCY / (n_gx * ROWS * n_gy * LANES)
    for g in range(groups):
        mean = jnp.sum(jnp.where(lane == sub + ROWS * g, own * scale, 0.0), axis=1, keepdims=True)
        for j in range(ROWS):
            rows = pl.ds(g * 64 + j, ROWS, stride=ROWS)
            out[2, rows, :] = out[2, rows, :] - mean

    for copy in first + second + third + y_copies + x_copies + c_copies:
        copy.wait_send()


def body(sizes, fields, coriolis, slope_east, slope_north):
    depth = fields.shape[1]
    nx, nl, nc, nh, nz = sizes
    cells = depth * ROWS
    halves = cells // LANES
    f32 = jnp.float32
    any_space = pl.BlockSpec(memory_space=pl.ANY)
    count_a, count_z, count_y = max(nx * nc - 1, 1), max(nz - 1, 1), max(nl * nh - 1, 1)
    dma = pltpu.SemaphoreType.DMA
    out = pl.pallas_call(
        functools.partial(kernel, sizes),
        out_shape=jax.ShapeDtypeStruct((4, cells, LANES), f32),
        in_specs=[any_space] * 4,
        out_specs=pl.BlockSpec(memory_space=pltpu.VMEM),
        scratch_shapes=[
            pltpu.VMEM((5, cells + 2 * EDGE, LANES), f32),
            pltpu.VMEM((5, halves, LANES + 2 * ROWS, LANES), f32),
            pltpu.VMEM((2, 13, depth, LANES), f32),
            pltpu.VMEM((2, 13, depth, LANES), f32),
            pltpu.VMEM((2, cells, LANES), f32),
            pltpu.VMEM((2, 2, depth, LANES), f32),
            pltpu.VMEM((2, 2, depth, LANES), f32),
            pltpu.VMEM((ROWS + 2, depth, LANES), f32),
            pltpu.VMEM((cells, LANES), f32),
            pltpu.VMEM((cells, LANES), f32),
            pltpu.VMEM((halves, LANES + 2 * ROWS, LANES), f32),
            pltpu.VMEM((4, halves, LANES, LANES), f32),
            pltpu.VMEM((ROWS, LANES), f32),
            pltpu.VMEM((ROWS, LANES), f32),
            pltpu.SMEM((ROWS,), f32),
            pltpu.VMEM((3, 1, LANES), f32),
            pltpu.VMEM((count_a, 1, LANES), f32),
            pltpu.VMEM((count_z, 1, LANES), f32),
            pltpu.VMEM((count_y, 1, LANES), f32),
            dma((8,)),
            dma((count_a,)), dma((count_a,)),
            dma((count_z,)), dma((count_z,)),
            dma((count_y,)), dma((count_y,)),
            dma((6,)), dma((6,)),
        ],
        compiler_params=pltpu.CompilerParams(collective_id=0, has_side_effects=True),
    )(fields.reshape(5, cells, LANES), coriolis, slope_east, slope_north)
    return out.reshape(4, depth, ROWS, LANES)


def solution(mesh):
    return build(mesh, (4, 2, 2, 4, 12))


def build(mesh, sizes):
    finer = Mesh(mesh.devices.reshape(sizes), AXES)
    in_specs = (P(None, None, GX, GY), P(GX), P(GX, GY), P(GX, GY))
    out_specs = P(None, None, GX, GY)
    step = functools.partial(body, sizes)
    return jax.shard_map(step, mesh=finer, in_specs=in_specs, out_specs=out_specs, check_vma=False)
```

```python
import functools

import jax
import jax.numpy as jnp
from jax import lax
from jax.experimental import pallas as pl
from jax.experimental.pallas import tpu as pltpu
from jax.sharding import Mesh
from jax.sharding import PartitionSpec as P

AXES = ("gx_0", "gx_1", "gx_2", "gy_0", "gy_1")
GX = ("gx_0", "gx_1", "gx_2")
GY = ("gy_0", "gy_1")
MESH = pl.DeviceIdType.MESH

WENO_EPS = 1e-06
SECTION_DT = 0.3
SMAG_COEF = 0.06
BACKGROUND = 0.05
BUOYANCY = 0.5

LANES = 128
ROWS = 8
NEAR_Z, NEAR_Y = 3, 2
EDGE = 24


def line_terms(q, sigma, size, upward, mixing):
    count = len(q) - 6
    g = [q[i + 1] - q[i] for i in range(count + 5)]
    bend = [g[i + 1] - g[i] for i in range(count + 4)]
    third = [bend[i + 1] - bend[i] for i in range(count + 3)]
    mid, low, high = [], [], []
    for i in range(count + 4):
        before, after, d = g[i], g[i + 1], bend[i]
        a = (d * (4.0 / 3.0)) * d + (before * after + WENO_EPS)
        d2 = d + d
        b = a + after * d2
        c = a - before * d2
        mid.append(a * a)
        low.append(b * b)
        high.append(c * c)
    out = []
    for f in range(count + 1):
        up = upward[f]
        e0 = jnp.where(up, low[f], high[f + 3])
        e1 = jnp.where(up, mid[f + 1], mid[f + 2])
        e2 = jnp.where(up, high[f + 2], low[f + 1])
        curve = jnp.where(up, bend[f + 1], bend[f + 2])
        t0 = jnp.where(up, third[f], third[f + 2])
        u = e0 * 3.0
        v = e2 + e2
        den = e1 * (e2 + u) + u * v
        num = e1 * (u * third[f + 1] + v * t0)
        flux = sigma[f] * ((q[f + 2] + q[f + 3]) - curve * (1.0 / 3.0)) + size[f] * (num / den)
        if mixing is not None:
            flux = flux + mixing[f] * g[f + 2]
        out.append(flux)
    return out


def speeds(s, keep_first=None, keep_last=None):
    count = len(s) - 6
    sigma = [(s[f + 2] + s[f + 3]) * (-0.25 * SECTION_DT) for f in range(count + 1)]
    if keep_first is not None:
        sigma[0] = jnp.where(keep_first, sigma[0], 0.0)
        sigma[count] = jnp.where(keep_last, sigma[count], 0.0)
    upward = [x < 0.0 for x in sigma]
    size = [jnp.abs(x) * (1.0 / 3.0) for x in sigma]
    return sigma, size, upward


def kernel(
    sizes, fields, coriolis, slope_east, slope_north, out,
    zf, xt, ysend, yrecv, halo, csend, crecv, eddy_y, eddy_z, eddy_v, eddy_x, xdiv, east, north, cor,
    row_send, recv_a, recv_z, recv_y,
    load_sem, send_a, got_a, send_z, got_z, send_y, got_y, send_h, got_h, vouch,
):
    nx, nl, nc, nh, nz = sizes
    ny = nh * nl
    n_gx, n_gy = nx * nl * nc, nh * nz
    depth = out.shape[1] // ROWS
    groups = depth // ROWS
    px, pl_, pc, ph, pz = (lax.axis_index(a) for a in AXES)
    py = ph * nl + pl_
    gx = (px * nl + pl_) * nc + pc
    gy = ph * nz + pz

    def at_gx(i):
        i = lax.rem(i + n_gx, n_gx)
        return (i // (nl * nc), lax.rem(i // nc, nl), lax.rem(i, nc), ph, pz)

    def at_gy(i):
        i = lax.rem(i + n_gy, n_gy)
        return (px, pl_, pc, i // nz, lax.rem(i, nz))

    peers_a = [
        (lax.rem(px + dx, nx), pl_, lax.rem(pc + dc, nc), ph, pz)
        for dx in range(nx)
        for dc in range(nc)
        if dx or dc
    ]

    def at_z(dz):
        return (px, pl_, pc, ph, lax.rem(pz + dz, nz))

    def at_y(dy):
        y = lax.rem(py + dy, ny)
        return (px, lax.rem(y, nl), pc, y // nl, pz)

    peers_z = [at_z(dz) for dz in range(1, nz)]
    peers_y = [at_y(dy) for dy in range(1, ny)]
    gx_low, gx_high = at_gx(gx - 1), at_gx(gx + 1)
    gy_low, gy_high = at_gy(gy - 1), at_gy(gy + 1)

    main = pl.ds(EDGE, depth * ROWS)
    loads = [
        pltpu.make_async_copy(fields.at[f], zf.at[f, main], load_sem.at[f]) for f in (3, 0, 1, 2, 4)
    ]
    loads.append(pltpu.make_async_copy(slope_east, east, load_sem.at[5]))
    loads.append(pltpu.make_async_copy(slope_north, north, load_sem.at[6]))
    loads.append(pltpu.make_async_copy(coriolis, cor, load_sem.at[7]))
    for copy in loads:
        copy.start()

    barrier = pltpu.get_barrier_semaphore()
    near_z = [at_z(d) for d in range(1, nz) if min(d, nz - d) <= NEAR_Z]
    near_y = [at_y(d) for d in range(1, ny) if min(d, ny - d) <= NEAR_Y]
    nearby = [*peers_a, *near_z, *near_y, gx_low, gx_high, gy_low, gy_high]
    for peer in nearby:
        pl.semaphore_signal(barrier, inc=1, device_id=peer, device_id_type=MESH)

    lane = lax.broadcasted_iota(jnp.int32, (ROWS, LANES), 1)
    sub = lax.broadcasted_iota(jnp.int32, (ROWS, LANES), 0)

    def strided(ref, f, first):
        return ref[f, pl.ds(first, ROWS, stride=ROWS), :]

    loads[0].wait()
    own = jnp.zeros((ROWS, LANES), jnp.float32)
    for g in range(groups):
        level = strided(zf, 3, EDGE + 64 * g)
        for j in range(1, ROWS):
            level = level + strided(zf, 3, EDGE + 64 * g + j)
        own = own + jnp.where(lane == sub + ROWS * g, jnp.sum(level, axis=1, keepdims=True), 0.0)
    own = jnp.sum(own, axis=0, keepdims=True)
    row_send[0] = own

    def remote(src, dst, send, got, peer):
        return pltpu.make_async_remote_copy(
            src_ref=src, dst_ref=dst, send_sem=send, recv_sem=got, device_id=peer, device_id_type=MESH
        )

    def phase(index, peers, dst, send, got):
        copies = [
            remote(row_send.at[index], dst.at[i], send.at[i], got.at[i], peer)
            for i, peer in enumerate(peers)
        ]
        for copy in copies:
            copy.start()
        return copies

    def total_of(copies, dst, value):
        for i, copy in enumerate(copies):
            copy.wait_recv()
        for i in range(len(copies)):
            value = value + dst[i]
        return value

    pl.semaphore_wait(barrier, len(nearby))
    first = phase(0, peers_a, recv_a, send_a, got_a)
    relay_z = [at_z(NEAR_Z), at_z(nz - NEAR_Z)] if nz > 2 * NEAR_Z else []
    relay_y = [at_y(NEAR_Y), at_y(ny - NEAR_Y)] if ny > 2 * NEAR_Y else []
    for i, peers in enumerate((relay_z, relay_y)):
        for peer in peers:
            pl.semaphore_signal(vouch.at[i], inc=1, device_id=peer, device_id_type=MESH)

    for copy in loads[1:]:
        copy.wait()

    for f in range(5):
        for r in range(3):
            slab = r * 4 + f
            if f == 4:
                if r:
                    continue
                slab = 12
            low_row, high_row = (r, 5 + r) if f < 4 else (0, 7)
            ysend[0, slab] = zf[f, pl.ds(EDGE + low_row, depth, stride=ROWS), :]
            ysend[1, slab] = zf[f, pl.ds(EDGE + high_row, depth, stride=ROWS), :]
        bottom = zf[f, pl.ds(EDGE, ROWS), :]
        top = zf[f, pl.ds(EDGE + (depth - 1) * ROWS, ROWS), :]
        for r in range(3):
            zf[f, pl.ds(r * ROWS, ROWS), :] = bottom
            zf[f, pl.ds(EDGE + (depth + r) * ROWS, ROWS), :] = top
    halves = depth * ROWS // LANES

    def turn(i, carry):
        f, half = i // halves, lax.rem(i, halves)
        block = zf[f, pl.ds(EDGE + half * LANES, LANES), :]
        xt[f, half, pl.ds(ROWS, LANES), :] = block.T
        return carry

    lax.fori_loop(0, 5 * halves, turn, 0)

    y_copies = [
        remote(ysend.at[0], yrecv.at[1], send_h.at[0], got_h.at[0], gx_low),
        remote(ysend.at[1], yrecv.at[0], send_h.at[1], got_h.at[1], gx_high),
    ]
    x_copies = [
        remote(xt.at[:, :, pl.ds(ROWS, ROWS)], xt.at[:, :, pl.ds(ROWS + LANES, ROWS)], send_h.at[2], got_h.at[2], gy_low),
        remote(xt.at[:, :, pl.ds(LANES, ROWS)], xt.at[:, :, pl.ds(0, ROWS)], send_h.at[3], got_h.at[3], gy_high),
    ]
    for copy in x_copies + y_copies:
        copy.start()

    turning = jnp.zeros((ROWS, LANES), jnp.float32)
    for j in range(ROWS):
        turning = jnp.where(sub == j, cor[j] * SECTION_DT, turning)

    def upright(c, carry):
        base = c * ROWS * ROWS

        def cells(f, first=0, count=ROWS + 6):
            return [zf[f, pl.ds(base + (first + i) * ROWS, ROWS), :] for i in range(count)]

        p = cells(4, 2, ROWS + 2)
        slope = [(p[i + 2] - p[i]) * (0.5 * SECTION_DT) for i in range(ROWS)]
        top_factor = 1.0 - (c * ROWS).astype(jnp.float32) / depth
        w = cells(2)
        sigma, size, upward = speeds(w, c > 0, c < groups - 1)
        for f in range(4):
            q = w if f == 2 else cells(f)
            flux = line_terms(q, sigma, size, upward, None)
            for i in range(ROWS):
                value = q[i + 3] + (flux[i + 1] - flux[i])
                rows = pl.ds(base + i * ROWS, ROWS)
                if f == 0:
                    tilt = slope[i] * (top_factor - (i + 0.5) / depth)
                    value = value + east[...] * tilt + turning * zf[1, pl.ds(base + EDGE + i * ROWS, ROWS), :]
                elif f == 1:
                    tilt = slope[i] * (top_factor - (i + 0.5) / depth)
                    value = value + north[...] * tilt - turning * zf[0, pl.ds(base + EDGE + i * ROWS, ROWS), :]
                elif f == 2:
                    warm = zf[3, pl.ds(base + EDGE + i * ROWS, ROWS), :]
                    value = value - slope[i] + warm * (SECTION_DT * BUOYANCY)
                out[f, rows, :] = value
        return carry

    lax.fori_loop(0, groups, upright, 0)

    own = total_of(first, recv_a, own)
    row_send[1] = own
    if relay_z:
        pl.semaphore_wait(vouch.at[0], 2)
    second = phase(1, peers_z, recv_z, send_z, got_z)
    for copy in x_copies:
        copy.wait_recv()

    edge_rows = jnp.zeros((5, halves, ROWS, LANES), jnp.float32)

    @pl.when(gy == 0)
    def _():
        xt[:, :, pl.ds(0, ROWS), :] = edge_rows

    @pl.when(gy == n_gy - 1)
    def _():
        xt[:, :, pl.ds(ROWS + LANES, ROWS), :] = edge_rows

    gap = jnp.zeros((LANES - 2 * ROWS, LANES), jnp.float32)
    for f in range(2):
        for half in range(halves):
            block = jnp.concatenate(
                [xt[f, half, pl.ds(ROWS + LANES, ROWS), :], gap, xt[f, half, pl.ds(0, ROWS), :]], axis=0
            )
            halo[f, pl.ds(half * LANES, LANES), :] = block.T
    for f in range(2):
        csend[0, f] = halo[f, pl.ds(0, depth, stride=ROWS), :]
        csend[1, f] = halo[f, pl.ds(7, depth, stride=ROWS), :]

    c_copies = [
        remote(csend.at[0], crecv.at[1], send_h.at[4], got_h.at[4], gx_low),
        remote(csend.at[1], crecv.at[0], send_h.at[5], got_h.at[5], gx_high),
    ]
    for copy in c_copies:
        copy.start()
    own = total_of(second, recv_z, own)
    row_send[2] = own
    if relay_y:
        pl.semaphore_wait(vouch.at[1], 2)
    third = phase(2, peers_y, recv_y, send_y, got_y)
    for copy in y_copies + c_copies:
        copy.wait_recv()

    for side, at_edge in ((0, gx == 0), (1, gx == n_gx - 1)):

        @pl.when(at_edge)
        def _():
            yrecv[side] = jnp.zeros(yrecv.shape[1:], jnp.float32)
            crecv[side] = jnp.zeros(crecv.shape[1:], jnp.float32)

    def row(f, j, g):
        if j < 0:
            return yrecv[0, (j + 3) * 4 + f if f < 4 else 12, pl.ds(g * ROWS, ROWS), :]
        if j >= ROWS:
            return yrecv[1, (j - ROWS) * 4 + f if f < 4 else 12, pl.ds(g * ROWS, ROWS), :]
        return strided(zf, f, EDGE + g * 64 + j)

    def halo_row(f, j, g):
        if j < 0:
            return crecv[0, f, pl.ds(g * ROWS, ROWS), :]
        if j >= ROWS:
            return crecv[1, f, pl.ds(g * ROWS, ROWS), :]
        return strided(halo, f, g * 64 + j)

    def strength(ux, vx, uy, vy):
        cross = uy + vx
        return SMAG_COEF * jnp.sqrt(0.5 * (ux * ux + vy * vy) + 0.25 * (cross * cross) + BACKGROUND)

    def eddies(g, carry):
        u = [row(0, j, g) for j in range(-2, ROWS + 2)]
        v = [row(1, j, g) for j in range(-2, ROWS + 2)]
        hu = [halo_row(0, j, g) for j in range(-1, ROWS + 1)]
        hv = [halo_row(1, j, g) for j in range(-1, ROWS + 1)]
        left, right = lane == LANES - 1, lane == 0

        def across(inner, outer):
            plus = pltpu.roll(jnp.where(right, outer, inner), LANES - 1, 1)
            minus = pltpu.roll(jnp.where(left, outer, inner), 1, 1)
            return plus - minus

        for j in range(-1, ROWS + 1):
            ux, vx = across(u[j + 2], hu[j + 1]), across(v[j + 2], hv[j + 1])
            uy, vy = u[j + 3] - u[j + 1], v[j + 3] - v[j + 1]
            e = strength(ux, vx, uy, vy)
            eddy_y[j + 1, pl.ds(g * ROWS, ROWS), :] = e
            if 0 <= j < ROWS:
                eddy_z[pl.ds(g * 64 + j, ROWS, stride=ROWS), :] = e
                ux, vx = across(hu[j + 1], u[j + 2]), across(hv[j + 1], v[j + 2])
                uy, vy = hu[j + 2] - hu[j], hv[j + 2] - hv[j]
                eddy_v[pl.ds(g * 64 + j, ROWS, stride=ROWS), :] = strength(ux, vx, uy, vy)
        return carry

    lax.fori_loop(0, groups, eddies, 0)
    for half in range(halves):
        eddy_x[half, pl.ds(ROWS, LANES), :] = eddy_z[pl.ds(half * LANES, LANES), :].T
        outer = eddy_v[pl.ds(half * LANES, LANES), :].T
        eddy_x[half, pl.ds(0, ROWS), :] = outer[LANES - ROWS :]
        eddy_x[half, pl.ds(ROWS + LANES, ROWS), :] = outer[:ROWS]

    def northward(g, carry):
        v = [row(1, j, g) for j in range(-3, ROWS + 3)]
        sigma, size, upward = speeds(v)
        e = [eddy_y[j, pl.ds(g * ROWS, ROWS), :] for j in range(ROWS + 2)]
        mixing = [(e[f] + e[f + 1]) * (0.5 * SECTION_DT) for f in range(ROWS + 1)]
        p = [row(4, j, g) for j in range(-1, ROWS + 1)]
        for f in range(4):
            q = v if f == 1 else [row(f, j, g) for j in range(-3, ROWS + 3)]
            flux = line_terms(q, sigma, size, upward, mixing)
            for j in range(ROWS):
                value = flux[j + 1] - flux[j]
                if f == 1:
                    value = value - (p[j + 2] - p[j]) * (0.5 * SECTION_DT)
                rows = pl.ds(g * 64 + j, ROWS, stride=ROWS)
                out[f, rows, :] = out[f, rows, :] + value
        return carry

    lax.fori_loop(0, groups, northward, 0)

    step = LANES // ROWS

    def eastward(c, carry):
        half, start = c // 2, lax.rem(c, 2) * ROWS

        def cells(f, first=-3, count=ROWS + 6):
            return [
                xt[f, half, pl.ds(start + (ROWS + first + i), ROWS, stride=step), :] for i in range(count)
            ]

        u = cells(0)
        sigma, size, upward = speeds(u)
        e = [eddy_x[half, pl.ds(start + (ROWS - 1 + i), ROWS, stride=step), :] for i in range(ROWS + 2)]
        mixing = [(e[f] + e[f + 1]) * (0.5 * SECTION_DT) for f in range(ROWS + 1)]
        p = cells(4, -1, ROWS + 2)
        for f in range(4):
            q = u if f == 0 else cells(f)
            flux = line_terms(q, sigma, size, upward, mixing)
            for i in range(ROWS):
                value = flux[i + 1] - flux[i]
                if f == 0:
                    value = value - (p[i + 2] - p[i]) * (0.5 * SECTION_DT)
                xdiv[f, half, pl.ds(start + i, ROWS, stride=step), :] = value
        return carry

    lax.fori_loop(0, 2 * halves, eastward, 0)

    def turn_back(i, carry):
        f, half = i // halves, lax.rem(i, halves)
        rows = pl.ds(half * LANES, LANES)
        out[f, rows, :] = out[f, rows, :] + xdiv[f, half].T
        return carry

    lax.fori_loop(0, 4 * halves, turn_back, 0)

    own = total_of(third, recv_y, own)
    scale = SECTION_DT * BUOYANCY / (n_gx * ROWS * n_gy * LANES)
    for g in range(groups):
        mean = jnp.sum(jnp.where(lane == sub + ROWS * g, own * scale, 0.0), axis=1, keepdims=True)
        for j in range(ROWS):
            rows = pl.ds(g * 64 + j, ROWS, stride=ROWS)
            out[2, rows, :] = out[2, rows, :] - mean

    for copy in first + second + third + y_copies + x_copies + c_copies:
        copy.wait_send()


def body(sizes, fields, coriolis, slope_east, slope_north):
    depth = fields.shape[1]
    nx, nl, nc, nh, nz = sizes
    cells = depth * ROWS
    halves = cells // LANES
    f32 = jnp.float32
    hbm = pl.BlockSpec(memory_space=pltpu.HBM)
    count_a, count_z, count_y = max(nx * nc - 1, 1), max(nz - 1, 1), max(nl * nh - 1, 1)
    dma = pltpu.SemaphoreType.DMA
    arrays = (fields.reshape(5, cells, LANES), coriolis, slope_east, slope_north)
    out = pl.pallas_call(
        functools.partial(kernel, sizes),
        out_shape=jax.ShapeDtypeStruct((4, cells, LANES), f32),
        in_specs=[hbm] * 4,
        out_specs=pl.BlockSpec(memory_space=pltpu.VMEM),
        scratch_shapes=[
            pltpu.VMEM((5, cells + 2 * EDGE, LANES), f32),
            pltpu.VMEM((5, halves, LANES + 2 * ROWS, LANES), f32),
            pltpu.VMEM((2, 13, depth, LANES), f32),
            pltpu.VMEM((2, 13, depth, LANES), f32),
            pltpu.VMEM((2, cells, LANES), f32),
            pltpu.VMEM((2, 2, depth, LANES), f32),
            pltpu.VMEM((2, 2, depth, LANES), f32),
            pltpu.VMEM((ROWS + 2, depth, LANES), f32),
            pltpu.VMEM((cells, LANES), f32),
            pltpu.VMEM((cells, LANES), f32),
            pltpu.VMEM((halves, LANES + 2 * ROWS, LANES), f32),
            pltpu.VMEM((4, halves, LANES, LANES), f32),
            pltpu.VMEM((ROWS, LANES), f32),
            pltpu.VMEM((ROWS, LANES), f32),
            pltpu.SMEM((ROWS,), f32),
            pltpu.VMEM((3, 1, LANES), f32),
            pltpu.VMEM((count_a, 1, LANES), f32),
            pltpu.VMEM((count_z, 1, LANES), f32),
            pltpu.VMEM((count_y, 1, LANES), f32),
            dma((8,)),
            dma((count_a,)), dma((count_a,)),
            dma((count_z,)), dma((count_z,)),
            dma((count_y,)), dma((count_y,)),
            dma((6,)), dma((6,)), pltpu.SemaphoreType.REGULAR((2,)),
        ],
        compiler_params=pltpu.CompilerParams(
            collective_id=0, has_side_effects=True, vmem_limit_bytes=24 * 1024 * 1024
        ),
    )(*(pltpu.with_memory_space_constraint(a, pltpu.HBM) for a in arrays))
    return out.reshape(4, depth, ROWS, LANES)


def solution(mesh):
    return build(mesh, (4, 2, 2, 4, 12))


def build(mesh, sizes):
    finer = Mesh(mesh.devices.reshape(sizes), AXES)
    in_specs = (P(None, None, GX, GY), P(GX), P(GX, GY), P(GX, GY))
    out_specs = P(None, None, GX, GY)
    step = functools.partial(body, sizes)
    return jax.shard_map(step, mesh=finer, in_specs=in_specs, out_specs=out_specs, check_vma=False)
```

```python
import functools

import jax
import jax.numpy as jnp
from jax import lax
from jax.experimental import pallas as pl
from jax.experimental.pallas import tpu as pltpu
from jax.sharding import Mesh
from jax.sharding import PartitionSpec as P

AXES = ("gx_0", "gx_1", "gx_2", "gy_0", "gy_1")
GX = ("gx_0", "gx_1", "gx_2")
GY = ("gy_0", "gy_1")
MESH = pl.DeviceIdType.MESH

WENO_EPS = 1e-06
SECTION_DT = 0.3
SMAG_COEF = 0.06
BACKGROUND = 0.05
BUOYANCY = 0.5

LANES = 128
ROWS = 8
NEAR_Z, NEAR_Y = 3, 2
EDGE = 24


def line_terms(q, sigma, size, upward, mixing):
    count = len(q) - 6
    g = [q[i + 1] - q[i] for i in range(count + 5)]
    bend = [g[i + 1] - g[i] for i in range(count + 4)]
    third = [bend[i + 1] - bend[i] for i in range(count + 3)]
    mid, low, high = [], [], []
    for i in range(count + 4):
        before, after, d = g[i], g[i + 1], bend[i]
        a = (d * (4.0 / 3.0)) * d + (before * after + WENO_EPS)
        d2 = d + d
        b = a + after * d2
        c = a - before * d2
        mid.append(a * a)
        low.append(b * b)
        high.append(c * c)
    out = []
    for f in range(count + 1):
        up = upward[f]
        e0 = jnp.where(up, low[f], high[f + 3])
        e1 = jnp.where(up, mid[f + 1], mid[f + 2])
        e2 = jnp.where(up, high[f + 2], low[f + 1])
        curve = jnp.where(up, bend[f + 1], bend[f + 2])
        t0 = jnp.where(up, third[f], third[f + 2])
        u = e0 * 3.0
        v = e2 + e2
        den = e1 * (e2 + u) + u * v
        num = e1 * (u * third[f + 1] + v * t0)
        flux = sigma[f] * ((q[f + 2] + q[f + 3]) - curve * (1.0 / 3.0)) + size[f] * (num / den)
        if mixing is not None:
            flux = flux + mixing[f] * g[f + 2]
        out.append(flux)
    return out


def speeds(s, keep_first=None, keep_last=None):
    count = len(s) - 6
    sigma = [(s[f + 2] + s[f + 3]) * (-0.25 * SECTION_DT) for f in range(count + 1)]
    if keep_first is not None:
        sigma[0] = jnp.where(keep_first, sigma[0], 0.0)
        sigma[count] = jnp.where(keep_last, sigma[count], 0.0)
    upward = [x < 0.0 for x in sigma]
    size = [jnp.abs(x) * (1.0 / 3.0) for x in sigma]
    return sigma, size, upward


def kernel(
    sizes, fields, coriolis, slope_east, slope_north, out,
    zf, xt, ysend, yrecv, halo, csend, crecv, eddy_y, eddy_z, eddy_v, eddy_x, xdiv, east, north, cor,
    row_send, recv_a, recv_z, recv_y,
    load_sem, send_a, got_a, send_z, got_z, send_y, got_y, send_h, got_h, vouch,
):
    nx, nl, nc, nh, nz = sizes
    ny = nh * nl
    n_gx, n_gy = nx * nl * nc, nh * nz
    depth = out.shape[1] // ROWS
    groups = depth // ROWS
    px, pl_, pc, ph, pz = (lax.axis_index(a) for a in AXES)
    py = ph * nl + pl_
    main = pl.ds(EDGE, depth * ROWS)
    loads = [
        pltpu.make_async_copy(fields.at[f], zf.at[f, main], load_sem.at[f]) for f in (3, 0, 1, 2, 4)
    ]
    loads.append(pltpu.make_async_copy(slope_east, east, load_sem.at[5]))
    loads.append(pltpu.make_async_copy(slope_north, north, load_sem.at[6]))
    loads.append(pltpu.make_async_copy(coriolis, cor, load_sem.at[7]))
    for copy in loads:
        copy.start()

    gx = (px * nl + pl_) * nc + pc
    gy = ph * nz + pz

    def carry(coordinate, size):
        over = coordinate >= size
        return jnp.where(over, coordinate - size, coordinate), over.astype(jnp.int32)

    def step_up(fast, sizes_fast):
        carried, moved = 1, []
        for coordinate, size in zip(fast, sizes_fast, strict=True):
            coordinate, carried = carry(coordinate + carried, size)
            moved.append(coordinate)
        return moved

    def step_down(fast, sizes_fast):
        flipped = [size - 1 - c for c, size in zip(fast, sizes_fast, strict=True)]
        return [size - 1 - c for c, size in zip(step_up(flipped, sizes_fast), sizes_fast, strict=True)]

    def along_gx(step):
        c, l, x = step((pc, pl_, px), (nc, nl, nx))
        return (x, l, c, ph, pz)

    def along_gy(step):
        z, h = step((pz, ph), (nz, nh))
        return (px, pl_, pc, h, z)

    def at_z(dz):
        return (px, pl_, pc, ph, carry(pz + dz, nz)[0])

    def at_y(dy):
        l, over = carry(pl_ + dy % nl, nl)
        return (px, l, pc, carry(ph + dy // nl + over, nh)[0], pz)

    peers_a = [
        (carry(px + dx, nx)[0], pl_, carry(pc + dc, nc)[0], ph, pz)
        for dx in range(nx)
        for dc in range(nc)
        if dx or dc
    ]
    peers_z = [at_z(dz) for dz in range(1, nz)]
    peers_y = [at_y(dy) for dy in range(1, ny)]
    gx_low, gx_high = along_gx(step_down), along_gx(step_up)
    gy_low, gy_high = along_gy(step_down), along_gy(step_up)

    barrier = pltpu.get_barrier_semaphore()
    near_z = [at_z(d) for d in range(1, nz) if min(d, nz - d) <= NEAR_Z]
    near_y = [at_y(d) for d in range(1, ny) if min(d, ny - d) <= NEAR_Y]
    nearby = [*peers_a, *near_z, *near_y, gx_low, gx_high, gy_low, gy_high]
    for peer in nearby:
        pl.semaphore_signal(barrier, inc=1, device_id=peer, device_id_type=MESH)

    lane = lax.broadcasted_iota(jnp.int32, (ROWS, LANES), 1)
    sub = lax.broadcasted_iota(jnp.int32, (ROWS, LANES), 0)

    def strided(ref, f, first):
        return ref[f, pl.ds(first, ROWS, stride=ROWS), :]

    loads[0].wait()
    own = jnp.zeros((ROWS, LANES), jnp.float32)
    for g in range(groups):
        level = strided(zf, 3, EDGE + 64 * g)
        for j in range(1, ROWS):
            level = level + strided(zf, 3, EDGE + 64 * g + j)
        own = own + jnp.where(lane == sub + ROWS * g, jnp.sum(level, axis=1, keepdims=True), 0.0)
    own = jnp.sum(own, axis=0, keepdims=True)
    row_send[0] = own

    def remote(src, dst, send, got, peer):
        return pltpu.make_async_remote_copy(
            src_ref=src, dst_ref=dst, send_sem=send, recv_sem=got, device_id=peer, device_id_type=MESH
        )

    def phase(index, peers, dst, send, got):
        copies = [
            remote(row_send.at[index], dst.at[i], send.at[i], got.at[i], peer)
            for i, peer in enumerate(peers)
        ]
        for copy in copies:
            copy.start()
        return copies

    def total_of(copies, dst, value):
        for i, copy in enumerate(copies):
            copy.wait_recv()
        for i in range(len(copies)):
            value = value + dst[i]
        return value

    for copy in loads[1:]:
        copy.wait()

    for f in range(5):
        for r in range(3):
            slab = r * 4 + f
            if f == 4:
                if r:
                    continue
                slab = 12
            low_row, high_row = (r, 5 + r) if f < 4 else (0, 7)
            ysend[0, slab] = zf[f, pl.ds(EDGE + low_row, depth, stride=ROWS), :]
            ysend[1, slab] = zf[f, pl.ds(EDGE + high_row, depth, stride=ROWS), :]
        bottom = zf[f, pl.ds(EDGE, ROWS), :]
        top = zf[f, pl.ds(EDGE + (depth - 1) * ROWS, ROWS), :]
        for r in range(3):
            zf[f, pl.ds(r * ROWS, ROWS), :] = bottom
            zf[f, pl.ds(EDGE + (depth + r) * ROWS, ROWS), :] = top
    halves = depth * ROWS // LANES

    for f in range(5):
        for half in range(halves):
            block = zf[f, pl.ds(EDGE + half * LANES, LANES), :]
            xt[f, half, pl.ds(ROWS, LANES), :] = block.T

    pl.semaphore_wait(barrier, len(nearby))
    first = phase(0, peers_a, recv_a, send_a, got_a)
    relay_z = [at_z(NEAR_Z), at_z(nz - NEAR_Z)] if nz > 2 * NEAR_Z else []
    relay_y = [at_y(NEAR_Y), at_y(ny - NEAR_Y)] if ny > 2 * NEAR_Y else []
    for i, peers in enumerate((relay_z, relay_y)):
        for peer in peers:
            pl.semaphore_signal(vouch.at[i], inc=1, device_id=peer, device_id_type=MESH)

    x_copies = [
        remote(xt.at[:, :, pl.ds(ROWS, ROWS)], xt.at[:, :, pl.ds(ROWS + LANES, ROWS)], send_h.at[2], got_h.at[2], gy_low),
        remote(xt.at[:, :, pl.ds(LANES, ROWS)], xt.at[:, :, pl.ds(0, ROWS)], send_h.at[3], got_h.at[3], gy_high),
    ]
    y_copies = [
        remote(ysend.at[0], yrecv.at[1], send_h.at[0], got_h.at[0], gx_low),
        remote(ysend.at[1], yrecv.at[0], send_h.at[1], got_h.at[1], gx_high),
    ]
    for copy in x_copies + y_copies:
        copy.start()

    turning = jnp.zeros((ROWS, LANES), jnp.float32)
    for j in range(ROWS):
        turning = jnp.where(sub == j, cor[j] * SECTION_DT, turning)

    def upright(c, carry):
        base = c * ROWS * ROWS

        def cells(f, first=0, count=ROWS + 6):
            return [zf[f, pl.ds(base + (first + i) * ROWS, ROWS), :] for i in range(count)]

        p = cells(4, 2, ROWS + 2)
        slope = [(p[i + 2] - p[i]) * (0.5 * SECTION_DT) for i in range(ROWS)]
        top_factor = 1.0 - (c * ROWS).astype(jnp.float32) / depth
        w = cells(2)
        sigma, size, upward = speeds(w, c > 0, c < groups - 1)
        for f in range(4):
            q = w if f == 2 else cells(f)
            flux = line_terms(q, sigma, size, upward, None)
            for i in range(ROWS):
                value = q[i + 3] + (flux[i + 1] - flux[i])
                rows = pl.ds(base + i * ROWS, ROWS)
                if f == 0:
                    tilt = slope[i] * (top_factor - (i + 0.5) / depth)
                    value = value + east[...] * tilt + turning * zf[1, pl.ds(base + EDGE + i * ROWS, ROWS), :]
                elif f == 1:
                    tilt = slope[i] * (top_factor - (i + 0.5) / depth)
                    value = value + north[...] * tilt - turning * zf[0, pl.ds(base + EDGE + i * ROWS, ROWS), :]
                elif f == 2:
                    warm = zf[3, pl.ds(base + EDGE + i * ROWS, ROWS), :]
                    value = value - slope[i] + warm * (SECTION_DT * BUOYANCY)
                out[f, rows, :] = value
        return carry

    lax.fori_loop(0, groups, upright, 0)

    own = total_of(first, recv_a, own)
    row_send[1] = own
    if relay_z:
        pl.semaphore_wait(vouch.at[0], 2)
    second = phase(1, peers_z, recv_z, send_z, got_z)
    for copy in x_copies:
        copy.wait_recv()

    edge_rows = jnp.zeros((5, halves, ROWS, LANES), jnp.float32)

    @pl.when(gy == 0)
    def _():
        xt[:, :, pl.ds(0, ROWS), :] = edge_rows

    @pl.when(gy == n_gy - 1)
    def _():
        xt[:, :, pl.ds(ROWS + LANES, ROWS), :] = edge_rows

    gap = jnp.zeros((LANES - 2 * ROWS, LANES), jnp.float32)
    for f in range(2):
        for half in range(halves):
            block = jnp.concatenate(
                [xt[f, half, pl.ds(ROWS + LANES, ROWS), :], gap, xt[f, half, pl.ds(0, ROWS), :]], axis=0
            )
            halo[f, pl.ds(half * LANES, LANES), :] = block.T
    for f in range(2):
        csend[0, f] = halo[f, pl.ds(0, depth, stride=ROWS), :]
        csend[1, f] = halo[f, pl.ds(7, depth, stride=ROWS), :]

    c_copies = [
        remote(csend.at[0], crecv.at[1], send_h.at[4], got_h.at[4], gx_low),
        remote(csend.at[1], crecv.at[0], send_h.at[5], got_h.at[5], gx_high),
    ]
    for copy in c_copies:
        copy.start()
    own = total_of(second, recv_z, own)
    row_send[2] = own
    if relay_y:
        pl.semaphore_wait(vouch.at[1], 2)
    third = phase(2, peers_y, recv_y, send_y, got_y)
    for copy in y_copies + c_copies:
        copy.wait_recv()

    for side, at_edge in ((0, gx == 0), (1, gx == n_gx - 1)):

        @pl.when(at_edge)
        def _():
            yrecv[side] = jnp.zeros(yrecv.shape[1:], jnp.float32)
            crecv[side] = jnp.zeros(crecv.shape[1:], jnp.float32)

    def row(f, j, g):
        if j < 0:
            return yrecv[0, (j + 3) * 4 + f if f < 4 else 12, pl.ds(g * ROWS, ROWS), :]
        if j >= ROWS:
            return yrecv[1, (j - ROWS) * 4 + f if f < 4 else 12, pl.ds(g * ROWS, ROWS), :]
        return strided(zf, f, EDGE + g * 64 + j)

    def halo_row(f, j, g):
        if j < 0:
            return crecv[0, f, pl.ds(g * ROWS, ROWS), :]
        if j >= ROWS:
            return crecv[1, f, pl.ds(g * ROWS, ROWS), :]
        return strided(halo, f, g * 64 + j)

    def strength(ux, vx, uy, vy):
        cross = uy + vx
        return SMAG_COEF * jnp.sqrt(0.5 * (ux * ux + vy * vy) + 0.25 * (cross * cross) + BACKGROUND)

    def eddies(g, carry):
        u = [row(0, j, g) for j in range(-2, ROWS + 2)]
        v = [row(1, j, g) for j in range(-2, ROWS + 2)]
        hu = [halo_row(0, j, g) for j in range(-1, ROWS + 1)]
        hv = [halo_row(1, j, g) for j in range(-1, ROWS + 1)]
        left, right = lane == LANES - 1, lane == 0

        def across(inner, outer):
            plus = pltpu.roll(jnp.where(right, outer, inner), LANES - 1, 1)
            minus = pltpu.roll(jnp.where(left, outer, inner), 1, 1)
            return plus - minus

        for j in range(-1, ROWS + 1):
            ux, vx = across(u[j + 2], hu[j + 1]), across(v[j + 2], hv[j + 1])
            uy, vy = u[j + 3] - u[j + 1], v[j + 3] - v[j + 1]
            e = strength(ux, vx, uy, vy)
            eddy_y[j + 1, pl.ds(g * ROWS, ROWS), :] = e
            if 0 <= j < ROWS:
                eddy_z[pl.ds(g * 64 + j, ROWS, stride=ROWS), :] = e
                ux, vx = across(hu[j + 1], u[j + 2]), across(hv[j + 1], v[j + 2])
                uy, vy = hu[j + 2] - hu[j], hv[j + 2] - hv[j]
                eddy_v[pl.ds(g * 64 + j, ROWS, stride=ROWS), :] = strength(ux, vx, uy, vy)
        return carry

    lax.fori_loop(0, groups, eddies, 0)
    for half in range(halves):
        eddy_x[half, pl.ds(ROWS, LANES), :] = eddy_z[pl.ds(half * LANES, LANES), :].T
        outer = eddy_v[pl.ds(half * LANES, LANES), :].T
        eddy_x[half, pl.ds(0, ROWS), :] = outer[LANES - ROWS :]
        eddy_x[half, pl.ds(ROWS + LANES, ROWS), :] = outer[:ROWS]

    def northward(g, carry):
        v = [row(1, j, g) for j in range(-3, ROWS + 3)]
        sigma, size, upward = speeds(v)
        e = [eddy_y[j, pl.ds(g * ROWS, ROWS), :] for j in range(ROWS + 2)]
        mixing = [(e[f] + e[f + 1]) * (0.5 * SECTION_DT) for f in range(ROWS + 1)]
        p = [row(4, j, g) for j in range(-1, ROWS + 1)]
        for f in range(4):
            q = v if f == 1 else [row(f, j, g) for j in range(-3, ROWS + 3)]
            flux = line_terms(q, sigma, size, upward, mixing)
            for j in range(ROWS):
                value = flux[j + 1] - flux[j]
                if f == 1:
                    value = value - (p[j + 2] - p[j]) * (0.5 * SECTION_DT)
                rows = pl.ds(g * 64 + j, ROWS, stride=ROWS)
                out[f, rows, :] = out[f, rows, :] + value
        return carry

    lax.fori_loop(0, groups, northward, 0)

    step = LANES // ROWS

    def eastward(c, carry):
        half, start = c // 2, lax.rem(c, 2) * ROWS

        def cells(f, first=-3, count=ROWS + 6):
            return [
                xt[f, half, pl.ds(start + (ROWS + first + i), ROWS, stride=step), :] for i in range(count)
            ]

        u = cells(0)
        sigma, size, upward = speeds(u)
        e = [eddy_x[half, pl.ds(start + (ROWS - 1 + i), ROWS, stride=step), :] for i in range(ROWS + 2)]
        mixing = [(e[f] + e[f + 1]) * (0.5 * SECTION_DT) for f in range(ROWS + 1)]
        p = cells(4, -1, ROWS + 2)
        for f in range(4):
            q = u if f == 0 else cells(f)
            flux = line_terms(q, sigma, size, upward, mixing)
            for i in range(ROWS):
                value = flux[i + 1] - flux[i]
                if f == 0:
                    value = value - (p[i + 2] - p[i]) * (0.5 * SECTION_DT)
                xdiv[f, half, pl.ds(start + i, ROWS, stride=step), :] = value
        return carry

    lax.fori_loop(0, 2 * halves, eastward, 0)

    for f in range(4):
        for half in range(halves):
            rows = pl.ds(half * LANES, LANES)
            out[f, rows, :] = out[f, rows, :] + xdiv[f, half].T

    own = total_of(third, recv_y, own)
    scale = SECTION_DT * BUOYANCY / (n_gx * ROWS * n_gy * LANES)
    for g in range(groups):
        mean = jnp.sum(jnp.where(lane == sub + ROWS * g, own * scale, 0.0), axis=1, keepdims=True)
        for j in range(ROWS):
            rows = pl.ds(g * 64 + j, ROWS, stride=ROWS)
            out[2, rows, :] = out[2, rows, :] - mean

    for copy in first + second + third + y_copies + x_copies + c_copies:
        copy.wait_send()


def body(sizes, fields, coriolis, slope_east, slope_north):
    depth = fields.shape[1]
    nx, nl, nc, nh, nz = sizes
    cells = depth * ROWS
    halves = cells // LANES
    f32 = jnp.float32
    hbm = pl.BlockSpec(memory_space=pltpu.HBM)
    count_a, count_z, count_y = max(nx * nc - 1, 1), max(nz - 1, 1), max(nl * nh - 1, 1)
    dma = pltpu.SemaphoreType.DMA
    arrays = (fields.reshape(5, cells, LANES), coriolis, slope_east, slope_north)
    out = pl.pallas_call(
        functools.partial(kernel, sizes),
        out_shape=jax.ShapeDtypeStruct((4, cells, LANES), f32),
        in_specs=[hbm] * 4,
        out_specs=pl.BlockSpec(memory_space=pltpu.VMEM),
        scratch_shapes=[
            pltpu.VMEM((5, cells + 2 * EDGE, LANES), f32),
            pltpu.VMEM((5, halves, LANES + 2 * ROWS, LANES), f32),
            pltpu.VMEM((2, 13, depth, LANES), f32),
            pltpu.VMEM((2, 13, depth, LANES), f32),
            pltpu.VMEM((2, cells, LANES), f32),
            pltpu.VMEM((2, 2, depth, LANES), f32),
            pltpu.VMEM((2, 2, depth, LANES), f32),
            pltpu.VMEM((ROWS + 2, depth, LANES), f32),
            pltpu.VMEM((cells, LANES), f32),
            pltpu.VMEM((cells, LANES), f32),
            pltpu.VMEM((halves, LANES + 2 * ROWS, LANES), f32),
            pltpu.VMEM((4, halves, LANES, LANES), f32),
            pltpu.VMEM((ROWS, LANES), f32),
            pltpu.VMEM((ROWS, LANES), f32),
            pltpu.SMEM((ROWS,), f32),
            pltpu.VMEM((3, 1, LANES), f32),
            pltpu.VMEM((count_a, 1, LANES), f32),
            pltpu.VMEM((count_z, 1, LANES), f32),
            pltpu.VMEM((count_y, 1, LANES), f32),
            dma((8,)),
            dma((count_a,)), dma((count_a,)),
            dma((count_z,)), dma((count_z,)),
            dma((count_y,)), dma((count_y,)),
            dma((6,)), dma((6,)), pltpu.SemaphoreType.REGULAR((2,)),
        ],
        compiler_params=pltpu.CompilerParams(
            collective_id=0, has_side_effects=True, vmem_limit_bytes=24 * 1024 * 1024
        ),
    )(*(pltpu.with_memory_space_constraint(a, pltpu.HBM) for a in arrays))
    return out.reshape(4, depth, ROWS, LANES)


def solution(mesh):
    return build(mesh, (4, 2, 2, 4, 12))


def build(mesh, sizes):
    finer = Mesh(mesh.devices.reshape(sizes), AXES)
    in_specs = (P(None, None, GX, GY), P(GX), P(GX, GY), P(GX, GY))
    out_specs = P(None, None, GX, GY)
    step = functools.partial(body, sizes)
    return jax.shard_map(step, mesh=finer, in_specs=in_specs, out_specs=out_specs, check_vma=False)
```

```python
import functools

import jax
import jax.numpy as jnp
from jax import lax
from jax.experimental import pallas as pl
from jax.experimental.pallas import tpu as pltpu
from jax.sharding import Mesh
from jax.sharding import PartitionSpec as P

AXES = ("gx_0", "gx_1", "gx_2", "gy_0", "gy_1")
GX = ("gx_0", "gx_1", "gx_2")
GY = ("gy_0", "gy_1")
MESH = pl.DeviceIdType.MESH

WENO_EPS = 1e-06
SECTION_DT = 0.3
SMAG_COEF = 0.06
BACKGROUND = 0.05
BUOYANCY = 0.5

LANES = 128
ROWS = 8
NEAR_Y = 2
EDGE = 24


def line_terms(q, sigma, size, upward):
    count = len(q) - 6
    g = [q[i + 1] - q[i] for i in range(count + 5)]
    bend = [g[i + 1] - g[i] for i in range(count + 4)]
    third = [bend[i + 1] - bend[i] for i in range(count + 3)]
    mid, low, high = [], [], []
    for i in range(count + 4):
        before, after, d = g[i], g[i + 1], bend[i]
        a = (d * (4.0 / 3.0)) * d + (before * after + WENO_EPS)
        d2 = d + d
        b = a + after * d2
        c = a - before * d2
        mid.append(a * a)
        low.append(b * b)
        high.append(c * c)
    out = []
    for f in range(count + 1):
        up = upward[f]
        e0 = jnp.where(up, low[f], high[f + 3])
        e1 = jnp.where(up, mid[f + 1], mid[f + 2])
        e2 = jnp.where(up, high[f + 2], low[f + 1])
        curve = jnp.where(up, bend[f + 1], bend[f + 2])
        t0 = jnp.where(up, third[f], third[f + 2])
        u = e0 * 3.0
        v = e2 + e2
        den = e1 * (e2 + u) + u * v
        num = e1 * (u * third[f + 1] + v * t0)
        flux = sigma[f] * ((q[f + 2] + q[f + 3]) - curve * (1.0 / 3.0)) + size[f] * (num / den)
        out.append(flux)
    return out


def speeds(s, keep_first=None, keep_last=None):
    count = len(s) - 6
    sigma = [(s[f + 2] + s[f + 3]) * (-0.25 * SECTION_DT) for f in range(count + 1)]
    if keep_first is not None:
        sigma[0] = jnp.where(keep_first, sigma[0], 0.0)
        sigma[count] = jnp.where(keep_last, sigma[count], 0.0)
    upward = [x < 0.0 for x in sigma]
    size = [jnp.abs(x) * (1.0 / 3.0) for x in sigma]
    return sigma, size, upward


def kernel(
    sizes, fields, coriolis, slope_east, slope_north, out,
    zf, xt, ysend, yrecv, halo, csend, crecv, eddy_y, eddy_z, eddy_v, eddy_x, xdiv, east, north, cor,
    recv_a, recv_z, recv_y,
    load_sem, send_a, got_a, send_z, got_z, send_y, got_y, send_h, got_h, vouch,
):
    nx, nl, nc, nh, nz = sizes
    ny = nh * nl
    n_gx, n_gy = nx * nl * nc, nh * nz
    depth = out.shape[1] // ROWS
    groups = depth // ROWS
    px, pl_, pc, ph, pz = (lax.axis_index(a) for a in AXES)
    py = ph * nl + pl_
    main = pl.ds(EDGE, depth * ROWS)
    winds = pl.ds(0, 3)
    loads = [
        pltpu.make_async_copy(fields.at[3], zf.at[3, main], load_sem.at[0]),
        pltpu.make_async_copy(fields.at[winds], zf.at[winds, main], load_sem.at[1]),
        pltpu.make_async_copy(fields.at[4], zf.at[4, main], load_sem.at[2]),
        pltpu.make_async_copy(slope_east, east, load_sem.at[3]),
        pltpu.make_async_copy(slope_north, north, load_sem.at[4]),
        pltpu.make_async_copy(coriolis, cor, load_sem.at[5]),
    ]
    for copy in loads:
        copy.start()

    gx = (px * nl + pl_) * nc + pc
    gy = ph * nz + pz

    def carry(coordinate, size):
        over = coordinate >= size
        return jnp.where(over, coordinate - size, coordinate), over.astype(jnp.int32)

    def step_up(fast, sizes_fast):
        carried, moved = 1, []
        for coordinate, size in zip(fast, sizes_fast, strict=True):
            coordinate, carried = carry(coordinate + carried, size)
            moved.append(coordinate)
        return moved

    def step_down(fast, sizes_fast):
        flipped = [size - 1 - c for c, size in zip(fast, sizes_fast, strict=True)]
        return [size - 1 - c for c, size in zip(step_up(flipped, sizes_fast), sizes_fast, strict=True)]

    def along_gx(step):
        c, l, x = step((pc, pl_, px), (nc, nl, nx))
        return (x, l, c, ph, pz)

    def along_gy(step):
        z, h = step((pz, ph), (nz, nh))
        return (px, pl_, pc, h, z)

    def at_a(i):
        x = lax.div(i, nc)
        return (x, pl_, i - x * nc, ph, pz)

    def at_z(i):
        return (px, pl_, pc, ph, i)

    def at_y(i):
        h = lax.div(i, nl)
        return (px, i - h * nl, pc, h, pz)

    n_a = nx * nc
    pa, py = px * nc + pc, ph * nl + pl_
    near_y = [carry(py + d, ny)[0] for d in range(1, ny) if min(d, ny - d) <= NEAR_Y]
    gx_low, gx_high = along_gx(step_down), along_gx(step_up)
    gy_low, gy_high = along_gy(step_down), along_gy(step_up)

    barrier = pltpu.get_barrier_semaphore()

    def one(condition):
        return condition.astype(jnp.int32)

    def each(first, last, visit):
        def step(i, unused):
            visit(i)
            return unused

        lax.fori_loop(first, last, step, 0)

    def tell(sem, peer):
        pl.semaphore_signal(sem, inc=1, device_id=peer, device_id_type=MESH)

    together = [at_y(y) for y in near_y] + [gx_low, gx_high]
    for peer in together:
        tell(barrier, peer)
    for i in range(1, n_a):
        tell(barrier, at_a(carry(pa + i, n_a)[0]))
    each(pz + 1, nz, lambda i: tell(barrier, at_z(i)))
    pl.when(pz == 0)(functools.partial(tell, barrier, gy_low))
    expected = len(together) + n_a - 1 + pz + one(pz == nz - 1)

    lane = lax.broadcasted_iota(jnp.int32, (ROWS, LANES), 1)
    sub = lax.broadcasted_iota(jnp.int32, (ROWS, LANES), 0)

    def strided(ref, f, first):
        return ref[f, pl.ds(first, ROWS, stride=ROWS), :]

    loads[0].wait()
    own = jnp.zeros((ROWS, LANES), jnp.float32)
    for g in range(groups):
        level = strided(zf, 3, EDGE + 64 * g)
        for j in range(1, ROWS):
            level = level + strided(zf, 3, EDGE + 64 * g + j)
        own = own + jnp.where(lane == sub + ROWS * g, jnp.sum(level, axis=1, keepdims=True), 0.0)
    own = jnp.sum(own, axis=0, keepdims=True)
    recv_a[pa] = own

    def remote(src, dst, send, got, peer):
        return pltpu.make_async_remote_copy(
            src_ref=src, dst_ref=dst, send_sem=send, recv_sem=got, device_id=peer, device_id_type=MESH
        )

    def send_row(rows, me, send, got, place):
        return lambda i: remote(rows.at[me], rows.at[me], send, got, place(i)).start()

    def others(rows):
        return rows.at[pl.ds(0, rows.shape[0] - 1)]

    def all_of(ref, sem):
        pltpu.make_async_copy(ref, ref, sem).wait()

    def total_of(rows, got):
        all_of(others(rows), got)
        value = rows[0]
        for i in range(1, rows.shape[0]):
            value = value + rows[i]
        return value

    for copy in loads[1:]:
        copy.wait()

    for f in range(5):
        for r in range(3):
            slab = r * 4 + f
            if f == 4:
                if r:
                    continue
                slab = 12
            low_row, high_row = (r, 5 + r) if f < 4 else (0, 7)
            ysend[0, slab] = zf[f, pl.ds(EDGE + low_row, depth, stride=ROWS), :]
            ysend[1, slab] = zf[f, pl.ds(EDGE + high_row, depth, stride=ROWS), :]
        bottom = zf[f, pl.ds(EDGE, ROWS), :]
        top = zf[f, pl.ds(EDGE + (depth - 1) * ROWS, ROWS), :]
        for r in range(3):
            zf[f, pl.ds(r * ROWS, ROWS), :] = bottom
            zf[f, pl.ds(EDGE + (depth + r) * ROWS, ROWS), :] = top
    halves = depth * ROWS // LANES

    for f in range(5):
        for half in range(halves):
            block = zf[f, pl.ds(EDGE + half * LANES, LANES), :]
            xt[f, half, pl.ds(ROWS, LANES), :] = block.T

    pl.semaphore_wait(barrier, expected)
    to_a = send_row(recv_a, pa, send_a, got_a, at_a)
    for i in range(1, n_a):
        to_a(carry(pa + i, n_a)[0])
    tile_low, tile_high = xt.at[:, :, pl.ds(ROWS, ROWS)], xt.at[:, :, pl.ds(LANES, ROWS)]
    past_low, past_high = xt.at[:, :, pl.ds(0, ROWS)], xt.at[:, :, pl.ds(ROWS + LANES, ROWS)]
    x_copies = [
        remote(tile_low, past_high, send_h.at[2], got_h.at[2], gy_low),
        remote(tile_high, past_low, send_h.at[3], got_h.at[3], gy_high),
    ]
    pl.when(pz == nz - 1)(x_copies[1].start)
    pl.when(pz > 0)(x_copies[0].start)
    remote(ysend.at[0], yrecv.at[1], send_h.at[0], got_h.at[0], gx_low).start()
    remote(ysend.at[1], yrecv.at[0], send_h.at[0], got_h.at[0], gx_high).start()
    pl.when(pz == nz - 1)(functools.partial(tell, vouch.at[1], gy_high))
    pl.when(pz > 0)(functools.partial(tell, vouch.at[0], gy_low))
    each(0, pz, lambda i: tell(vouch.at[2], at_z(i)))
    far_y = ny > 2 * NEAR_Y
    if far_y:
        for d in (NEAR_Y, ny - NEAR_Y):
            tell(vouch.at[3], at_y(carry(py + d, ny)[0]))

    turning = jnp.zeros((ROWS, LANES), jnp.float32)
    for j in range(ROWS):
        turning = jnp.where(sub == j, cor[j] * SECTION_DT, turning)

    def upright(c, carry):
        base = c * ROWS * ROWS

        def cells(f, first=0, count=ROWS + 6):
            return [zf[f, pl.ds(base + (first + i) * ROWS, ROWS), :] for i in range(count)]

        p = cells(4, 2, ROWS + 2)
        slope = [(p[i + 2] - p[i]) * (0.5 * SECTION_DT) for i in range(ROWS)]
        top_factor = 1.0 - (c * ROWS).astype(jnp.float32) / depth
        w = cells(2)
        sigma, size, upward = speeds(w, c > 0, c < groups - 1)
        for f in range(4):
            q = w if f == 2 else cells(f)
            flux = line_terms(q, sigma, size, upward)
            for i in range(ROWS):
                value = q[i + 3] + (flux[i + 1] - flux[i])
                rows = pl.ds(base + i * ROWS, ROWS)
                if f == 0:
                    tilt = slope[i] * (top_factor - (i + 0.5) / depth)
                    value = value + east[...] * tilt + turning * zf[1, pl.ds(base + EDGE + i * ROWS, ROWS), :]
                elif f == 1:
                    tilt = slope[i] * (top_factor - (i + 0.5) / depth)
                    value = value + north[...] * tilt - turning * zf[0, pl.ds(base + EDGE + i * ROWS, ROWS), :]
                elif f == 2:
                    warm = zf[3, pl.ds(base + EDGE + i * ROWS, ROWS), :]
                    value = value - slope[i] + warm * (SECTION_DT * BUOYANCY)
                out[f, rows, :] = value
        return carry

    lax.fori_loop(0, groups, upright, 0)

    recv_z[pz] = total_of(recv_a, got_a)
    to_z = send_row(recv_z, pz, send_z, got_z, at_z)
    each(0, pz, to_z)

    @pl.when(pz < nz - 1)
    def _():
        pl.semaphore_wait(vouch.at[0], 1)
        x_copies[1].start()

    @pl.when(pz < nz - 1)
    def _():
        pl.semaphore_wait(vouch.at[2], nz - 1 - pz)
        each(pz + 1, nz, to_z)

    @pl.when(pz == 0)
    def _():
        pl.semaphore_wait(vouch.at[1], 1)
        x_copies[0].start()

    for copy in x_copies:
        copy.wait_recv()

    edge_rows = jnp.zeros((5, halves, ROWS, LANES), jnp.float32)

    @pl.when(gy == 0)
    def _():
        xt[:, :, pl.ds(0, ROWS), :] = edge_rows

    @pl.when(gy == n_gy - 1)
    def _():
        xt[:, :, pl.ds(ROWS + LANES, ROWS), :] = edge_rows

    gap = jnp.zeros((LANES - 2 * ROWS, LANES), jnp.float32)
    for f in range(2):
        for half in range(halves):
            block = jnp.concatenate(
                [xt[f, half, pl.ds(ROWS + LANES, ROWS), :], gap, xt[f, half, pl.ds(0, ROWS), :]], axis=0
            )
            halo[f, pl.ds(half * LANES, LANES), :] = block.T
    for f in range(2):
        csend[0, f] = halo[f, pl.ds(0, depth, stride=ROWS), :]
        csend[1, f] = halo[f, pl.ds(7, depth, stride=ROWS), :]

    remote(csend.at[0], crecv.at[1], send_h.at[1], got_h.at[1], gx_low).start()
    remote(csend.at[1], crecv.at[0], send_h.at[1], got_h.at[1], gx_high).start()
    step = LANES // ROWS

    def eastward(c, carry):
        half, start = c // 2, lax.rem(c, 2) * ROWS

        def cells(f, first=-3, count=ROWS + 6):
            return [
                xt[f, half, pl.ds(start + (ROWS + first + i), ROWS, stride=step), :] for i in range(count)
            ]

        u = cells(0)
        sigma, size, upward = speeds(u)
        p = cells(4, -1, ROWS + 2)
        for f in range(4):
            q = u if f == 0 else cells(f)
            flux = line_terms(q, sigma, size, upward)
            for i in range(ROWS):
                value = flux[i + 1] - flux[i]
                if f == 0:
                    value = value - (p[i + 2] - p[i]) * (0.5 * SECTION_DT)
                xdiv[f, half, pl.ds(start + i, ROWS, stride=step), :] = value
        return carry

    lax.fori_loop(0, 2 * halves, eastward, 0)

    all_of(yrecv, got_h.at[0])
    for side, at_edge in ((0, gx == 0), (1, gx == n_gx - 1)):

        @pl.when(at_edge)
        def _():
            yrecv[side] = jnp.zeros(yrecv.shape[1:], jnp.float32)

    def row(f, j, g):
        if j < 0:
            return yrecv[0, (j + 3) * 4 + f if f < 4 else 12, pl.ds(g * ROWS, ROWS), :]
        if j >= ROWS:
            return yrecv[1, (j - ROWS) * 4 + f if f < 4 else 12, pl.ds(g * ROWS, ROWS), :]
        return strided(zf, f, EDGE + g * 64 + j)

    def halo_row(f, j, g):
        if j < 0:
            return crecv[0, f, pl.ds(g * ROWS, ROWS), :]
        if j >= ROWS:
            return crecv[1, f, pl.ds(g * ROWS, ROWS), :]
        return strided(halo, f, g * 64 + j)

    def strength(ux, vx, uy, vy):
        cross = uy + vx
        return SMAG_COEF * jnp.sqrt(0.5 * (ux * ux + vy * vy) + 0.25 * (cross * cross) + BACKGROUND)

    def northward(g, carry):
        v = [row(1, j, g) for j in range(-3, ROWS + 3)]
        sigma, size, upward = speeds(v)
        p = [row(4, j, g) for j in range(-1, ROWS + 1)]
        for f in range(4):
            q = v if f == 1 else [row(f, j, g) for j in range(-3, ROWS + 3)]
            flux = line_terms(q, sigma, size, upward)
            for j in range(ROWS):
                value = flux[j + 1] - flux[j]
                if f == 1:
                    value = value - (p[j + 2] - p[j]) * (0.5 * SECTION_DT)
                rows = pl.ds(g * 64 + j, ROWS, stride=ROWS)
                out[f, rows, :] = out[f, rows, :] + value
        return carry

    lax.fori_loop(0, groups, northward, 0)

    recv_y[py] = total_of(recv_z, got_z)
    if far_y:
        pl.semaphore_wait(vouch.at[3], 2)
    to_y = send_row(recv_y, py, send_y, got_y, at_y)
    for i in range(1, ny):
        to_y(carry(py + i, ny)[0])

    all_of(crecv, got_h.at[1])
    for side, at_edge in ((0, gx == 0), (1, gx == n_gx - 1)):

        @pl.when(at_edge)
        def _():
            crecv[side] = jnp.zeros(crecv.shape[1:], jnp.float32)

    def eddies(g, carry):
        u = [row(0, j, g) for j in range(-2, ROWS + 2)]
        v = [row(1, j, g) for j in range(-2, ROWS + 2)]
        hu = [halo_row(0, j, g) for j in range(-1, ROWS + 1)]
        hv = [halo_row(1, j, g) for j in range(-1, ROWS + 1)]
        left, right = lane == LANES - 1, lane == 0

        def across(inner, outer):
            plus = pltpu.roll(jnp.where(right, outer, inner), LANES - 1, 1)
            minus = pltpu.roll(jnp.where(left, outer, inner), 1, 1)
            return plus - minus

        for j in range(-1, ROWS + 1):
            ux, vx = across(u[j + 2], hu[j + 1]), across(v[j + 2], hv[j + 1])
            uy, vy = u[j + 3] - u[j + 1], v[j + 3] - v[j + 1]
            e = strength(ux, vx, uy, vy)
            eddy_y[j + 1, pl.ds(g * ROWS, ROWS), :] = e
            if 0 <= j < ROWS:
                eddy_z[pl.ds(g * 64 + j, ROWS, stride=ROWS), :] = e
                ux, vx = across(hu[j + 1], u[j + 2]), across(hv[j + 1], v[j + 2])
                uy, vy = hu[j + 2] - hu[j], hv[j + 2] - hv[j]
                eddy_v[pl.ds(g * 64 + j, ROWS, stride=ROWS), :] = strength(ux, vx, uy, vy)
        return carry

    lax.fori_loop(0, groups, eddies, 0)
    for half in range(halves):
        eddy_x[half, pl.ds(ROWS, LANES), :] = eddy_z[pl.ds(half * LANES, LANES), :].T
        outer = eddy_v[pl.ds(half * LANES, LANES), :].T
        eddy_x[half, pl.ds(0, ROWS), :] = outer[LANES - ROWS :]
        eddy_x[half, pl.ds(ROWS + LANES, ROWS), :] = outer[:ROWS]

    def mix(e, q, add):
        count = len(e) - 2
        half_sum = [(e[i] + e[i + 1]) * (0.5 * SECTION_DT) for i in range(count + 1)]
        for f in range(4):
            line = q(f)
            flux = [half_sum[i] * (line[i + 1] - line[i]) for i in range(count + 1)]
            for i in range(count):
                add(f, i, flux[i + 1] - flux[i])

    def mix_north(g, carry):
        def add(f, j, value):
            rows = pl.ds(g * 64 + j, ROWS, stride=ROWS)
            out[f, rows, :] = out[f, rows, :] + value

        e = [eddy_y[j, pl.ds(g * ROWS, ROWS), :] for j in range(ROWS + 2)]
        mix(e, lambda f: [row(f, j, g) for j in range(-1, ROWS + 1)], add)
        return carry

    lax.fori_loop(0, groups, mix_north, 0)

    def mix_east(c, carry):
        half, start = c // 2, lax.rem(c, 2) * ROWS

        def line(ref, *lead):
            return [ref[*lead, half, pl.ds(start + (ROWS - 1 + i), ROWS, stride=step), :] for i in range(ROWS + 2)]

        def add(f, i, value):
            rows = pl.ds(start + i, ROWS, stride=step)
            xdiv[f, half, rows, :] = xdiv[f, half, rows, :] + value

        mix(line(eddy_x), lambda f: line(xt, f), add)
        return carry

    lax.fori_loop(0, 2 * halves, mix_east, 0)

    for f in range(4):
        for half in range(halves):
            rows = pl.ds(half * LANES, LANES)
            out[f, rows, :] = out[f, rows, :] + xdiv[f, half].T

    own = total_of(recv_y, got_y)
    scale = SECTION_DT * BUOYANCY / (n_gx * ROWS * n_gy * LANES)
    for g in range(groups):
        mean = jnp.sum(jnp.where(lane == sub + ROWS * g, own * scale, 0.0), axis=1, keepdims=True)
        for j in range(ROWS):
            rows = pl.ds(g * 64 + j, ROWS, stride=ROWS)
            out[2, rows, :] = out[2, rows, :] - mean

    for ref, sem in (
        (others(recv_a), send_a),
        (others(recv_z), send_z),
        (others(recv_y), send_y),
        (ysend, send_h.at[0]),
        (csend, send_h.at[1]),
    ):
        all_of(ref, sem)
    for copy in x_copies:
        copy.wait_send()


def body(sizes, fields, coriolis, slope_east, slope_north):
    depth = fields.shape[1]
    nx, nl, nc, nh, nz = sizes
    cells = depth * ROWS
    halves = cells // LANES
    f32 = jnp.float32
    hbm = pl.BlockSpec(memory_space=pltpu.HBM)
    dma = pltpu.SemaphoreType.DMA
    arrays = (fields.reshape(5, cells, LANES), coriolis, slope_east, slope_north)
    out = pl.pallas_call(
        functools.partial(kernel, sizes),
        out_shape=jax.ShapeDtypeStruct((4, cells, LANES), f32),
        in_specs=[hbm] * 4,
        out_specs=pl.BlockSpec(memory_space=pltpu.VMEM),
        scratch_shapes=[
            pltpu.VMEM((5, cells + 2 * EDGE, LANES), f32),
            pltpu.VMEM((5, halves, LANES + 2 * ROWS, LANES), f32),
            pltpu.VMEM((2, 13, depth, LANES), f32),
            pltpu.VMEM((2, 13, depth, LANES), f32),
            pltpu.VMEM((2, cells, LANES), f32),
            pltpu.VMEM((2, 2, depth, LANES), f32),
            pltpu.VMEM((2, 2, depth, LANES), f32),
            pltpu.VMEM((ROWS + 2, depth, LANES), f32),
            pltpu.VMEM((cells, LANES), f32),
            pltpu.VMEM((cells, LANES), f32),
            pltpu.VMEM((halves, LANES + 2 * ROWS, LANES), f32),
            pltpu.VMEM((4, halves, LANES, LANES), f32),
            pltpu.VMEM((ROWS, LANES), f32),
            pltpu.VMEM((ROWS, LANES), f32),
            pltpu.SMEM((ROWS,), f32),
            pltpu.VMEM((nx * nc, 1, LANES), f32),
            pltpu.VMEM((nz, 1, LANES), f32),
            pltpu.VMEM((nl * nh, 1, LANES), f32),
            dma((6,)), dma, dma, dma, dma, dma, dma, dma((4,)), dma((4,)),
            pltpu.SemaphoreType.REGULAR((4,)),
        ],
        compiler_params=pltpu.CompilerParams(
            collective_id=0, has_side_effects=True, vmem_limit_bytes=24 * 1024 * 1024
        ),
    )(*(pltpu.with_memory_space_constraint(a, pltpu.HBM) for a in arrays))
    return out.reshape(4, depth, ROWS, LANES)


def solution(mesh):
    return build(mesh, (4, 2, 2, 4, 12))


def build(mesh, sizes):
    finer = Mesh(mesh.devices.reshape(sizes), AXES)
    in_specs = (P(None, None, GX, GY), P(GX), P(GX, GY), P(GX, GY))
    out_specs = P(None, None, GX, GY)
    step = functools.partial(body, sizes)
    return jax.shard_map(step, mesh=finer, in_specs=in_specs, out_specs=out_specs, check_vma=False)
```

```python
import functools

import jax
import jax.numpy as jnp
from jax import lax
from jax.experimental import pallas as pl
from jax.experimental.pallas import tpu as pltpu
from jax.sharding import Mesh
from jax.sharding import PartitionSpec as P

AXES = ("gx_0", "gx_1", "gx_2", "gy_0", "gy_1")
GX = ("gx_0", "gx_1", "gx_2")
GY = ("gy_0", "gy_1")
MESH = pl.DeviceIdType.MESH

WENO_EPS = 1e-06
SECTION_DT = 0.3
SMAG_COEF = 0.06
BACKGROUND = 0.05
BUOYANCY = 0.5

LANES = 128
ROWS = 8
NEAR_Y = 2
EDGE = 24


def line_terms(q, sigma, size, upward):
    count = len(q) - 6
    g = [q[i + 1] - q[i] for i in range(count + 5)]
    bend = [g[i + 1] - g[i] for i in range(count + 4)]
    third = [bend[i + 1] - bend[i] for i in range(count + 3)]
    mid, low, high = [], [], []
    for i in range(count + 4):
        before, after, d = g[i], g[i + 1], bend[i]
        a = (d * (4.0 / 3.0)) * d + (before * after + WENO_EPS)
        d2 = d + d
        b = a + after * d2
        c = a - before * d2
        mid.append(a * a)
        low.append(b * b)
        high.append(c * c)
    out = []
    for f in range(count + 1):
        up = upward[f]
        e0 = jnp.where(up, low[f], high[f + 3])
        e1 = jnp.where(up, mid[f + 1], mid[f + 2])
        e2 = jnp.where(up, high[f + 2], low[f + 1])
        curve = jnp.where(up, bend[f + 1], bend[f + 2])
        t0 = jnp.where(up, third[f], third[f + 2])
        u = e0 * 3.0
        v = e2 + e2
        den = e1 * (e2 + u) + u * v
        num = e1 * (u * third[f + 1] + v * t0)
        flux = sigma[f] * ((q[f + 2] + q[f + 3]) - curve * (1.0 / 3.0)) + size[f] * (num / den)
        out.append(flux)
    return out


def speeds(s, keep_first=None, keep_last=None):
    count = len(s) - 6
    sigma = [(s[f + 2] + s[f + 3]) * (-0.25 * SECTION_DT) for f in range(count + 1)]
    if keep_first is not None:
        sigma[0] = jnp.where(keep_first, sigma[0], 0.0)
        sigma[count] = jnp.where(keep_last, sigma[count], 0.0)
    upward = [x < 0.0 for x in sigma]
    size = [jnp.abs(x) * (1.0 / 3.0) for x in sigma]
    return sigma, size, upward


def kernel(
    sizes, fields, coriolis, slope_east, slope_north, out,
    zf, xt, ysend, yrecv, halo, csend, crecv, eddy_y, eddy_z, eddy_v, eddy_x, xdiv, east, north, cor,
    recv_a, recv_q,
    load_sem, send_a, got_a, send_q, got_q, send_h, got_h, vouch,
):
    nx, nl, nc, nh, nz = sizes
    ny = nh * nl
    n_gx, n_gy = nx * nl * nc, nh * nz
    depth = out.shape[1] // ROWS
    groups = depth // ROWS
    px, pl_, pc, ph, pz = (lax.axis_index(a) for a in AXES)
    py = ph * nl + pl_
    main = pl.ds(EDGE, depth * ROWS)
    winds = pl.ds(0, 3)
    loads = [
        pltpu.make_async_copy(fields.at[3], zf.at[3, main], load_sem.at[0]),
        pltpu.make_async_copy(fields.at[winds], zf.at[winds, main], load_sem.at[1]),
        pltpu.make_async_copy(fields.at[4], zf.at[4, main], load_sem.at[2]),
        pltpu.make_async_copy(slope_east, east, load_sem.at[3]),
        pltpu.make_async_copy(slope_north, north, load_sem.at[4]),
        pltpu.make_async_copy(coriolis, cor, load_sem.at[5]),
    ]
    for copy in loads:
        copy.start()

    gx = (px * nl + pl_) * nc + pc
    gy = ph * nz + pz

    def carry(coordinate, size):
        over = coordinate >= size
        return jnp.where(over, coordinate - size, coordinate), over.astype(jnp.int32)

    def step_up(fast, sizes_fast):
        carried, moved = 1, []
        for coordinate, size in zip(fast, sizes_fast, strict=True):
            coordinate, carried = carry(coordinate + carried, size)
            moved.append(coordinate)
        return moved

    def step_down(fast, sizes_fast):
        flipped = [size - 1 - c for c, size in zip(fast, sizes_fast, strict=True)]
        return [size - 1 - c for c, size in zip(step_up(flipped, sizes_fast), sizes_fast, strict=True)]

    def along_gx(step):
        c, l, x = step((pc, pl_, px), (nc, nl, nx))
        return (x, l, c, ph, pz)

    def along_gy(step):
        z, h = step((pz, ph), (nz, nh))
        return (px, pl_, pc, h, z)

    def at_a(i):
        x = lax.div(i, nc)
        return (x, pl_, i - x * nc, ph, pz)

    def at_z(i):
        return (px, pl_, pc, ph, i)

    def at_y(i):
        h = lax.div(i, nl)
        return (px, i - h * nl, pc, h, pz)

    def at_q(y, z):
        return (*at_y(y)[:4], z)

    n_a = nx * nc
    pa, py = px * nc + pc, ph * nl + pl_
    pq = py * nz + pz
    around = [(min(d, ny - d) <= NEAR_Y, carry(py + d, ny)[0]) for d in range(1, ny)]
    near_y, far_y = [y for near, y in around if near], [y for near, y in around if not near]
    gx_low, gx_high = along_gx(step_down), along_gx(step_up)
    gy_low, gy_high = along_gy(step_down), along_gy(step_up)

    barrier = pltpu.get_barrier_semaphore()

    def one(condition):
        return condition.astype(jnp.int32)

    def each(first, last, visit):
        def step(i, unused):
            visit(i)
            return unused

        lax.fori_loop(first, last, step, 0)

    def tell(sem, peer):
        pl.semaphore_signal(sem, inc=1, device_id=peer, device_id_type=MESH)

    together = [at_y(y) for y in near_y] + [gx_low, gx_high]
    for peer in together:
        tell(barrier, peer)
    for i in range(1, n_a):
        tell(barrier, at_a(carry(pa + i, n_a)[0]))
    each(pz + 1, nz, lambda i: tell(barrier, at_z(i)))
    pl.when(pz == 0)(functools.partial(tell, barrier, gy_low))
    expected = len(together) + n_a - 1 + pz + one(pz == nz - 1)

    lane = lax.broadcasted_iota(jnp.int32, (ROWS, LANES), 1)
    sub = lax.broadcasted_iota(jnp.int32, (ROWS, LANES), 0)

    def strided(ref, f, first):
        return ref[f, pl.ds(first, ROWS, stride=ROWS), :]

    loads[0].wait()
    own = jnp.zeros((ROWS, LANES), jnp.float32)
    for g in range(groups):
        level = strided(zf, 3, EDGE + 64 * g)
        for j in range(1, ROWS):
            level = level + strided(zf, 3, EDGE + 64 * g + j)
        own = own + jnp.where(lane == sub + ROWS * g, jnp.sum(level, axis=1, keepdims=True), 0.0)
    own = jnp.sum(own, axis=0, keepdims=True)
    recv_a[pa] = own

    def remote(src, dst, send, got, peer):
        return pltpu.make_async_remote_copy(
            src_ref=src, dst_ref=dst, send_sem=send, recv_sem=got, device_id=peer, device_id_type=MESH
        )

    def send_row(rows, me, send, got, place):
        return lambda i: remote(rows.at[me], rows.at[me], send, got, place(i)).start()

    def others(rows):
        return rows.at[pl.ds(0, rows.shape[0] - 1)]

    def all_of(ref, sem):
        pltpu.make_async_copy(ref, ref, sem).wait()

    def total_of(rows, got):
        all_of(others(rows), got)
        parts = [rows[i] for i in range(rows.shape[0])]
        while len(parts) > 1:
            parts = [sum(parts[i : i + 2][1:], parts[i]) for i in range(0, len(parts), 2)]
        return parts[0]

    for copy in loads[1:]:
        copy.wait()

    for f in range(5):
        for r in range(3):
            slab = r * 4 + f
            if f == 4:
                if r:
                    continue
                slab = 12
            low_row, high_row = (r, 5 + r) if f < 4 else (0, 7)
            ysend[0, slab] = zf[f, pl.ds(EDGE + low_row, depth, stride=ROWS), :]
            ysend[1, slab] = zf[f, pl.ds(EDGE + high_row, depth, stride=ROWS), :]
        bottom = zf[f, pl.ds(EDGE, ROWS), :]
        top = zf[f, pl.ds(EDGE + (depth - 1) * ROWS, ROWS), :]
        for r in range(3):
            zf[f, pl.ds(r * ROWS, ROWS), :] = bottom
            zf[f, pl.ds(EDGE + (depth + r) * ROWS, ROWS), :] = top
    halves = depth * ROWS // LANES

    for f in range(5):
        for half in range(halves):
            block = zf[f, pl.ds(EDGE + half * LANES, LANES), :]
            xt[f, half, pl.ds(ROWS, LANES), :] = block.T

    pl.semaphore_wait(barrier, expected)
    to_a = send_row(recv_a, pa, send_a, got_a, at_a)
    for i in range(1, n_a):
        to_a(carry(pa + i, n_a)[0])
    tile_low, tile_high = xt.at[:, :, pl.ds(ROWS, ROWS)], xt.at[:, :, pl.ds(LANES, ROWS)]
    past_low, past_high = xt.at[:, :, pl.ds(0, ROWS)], xt.at[:, :, pl.ds(ROWS + LANES, ROWS)]
    x_copies = [
        remote(tile_low, past_high, send_h.at[2], got_h.at[2], gy_low),
        remote(tile_high, past_low, send_h.at[3], got_h.at[3], gy_high),
    ]
    pl.when(pz == nz - 1)(x_copies[1].start)
    pl.when(pz > 0)(x_copies[0].start)
    remote(ysend.at[0], yrecv.at[1], send_h.at[0], got_h.at[0], gx_low).start()
    remote(ysend.at[1], yrecv.at[0], send_h.at[0], got_h.at[0], gx_high).start()
    pl.when(pz == nz - 1)(functools.partial(tell, vouch.at[1], gy_high))
    pl.when(pz > 0)(functools.partial(tell, vouch.at[0], gy_low))
    for y in near_y:
        tell(vouch.at[2], at_y(y))

    turning = jnp.zeros((ROWS, LANES), jnp.float32)
    for j in range(ROWS):
        turning = jnp.where(sub == j, cor[j] * SECTION_DT, turning)

    def upright(c, carry):
        base = c * ROWS * ROWS

        def cells(f, first=0, count=ROWS + 6):
            return [zf[f, pl.ds(base + (first + i) * ROWS, ROWS), :] for i in range(count)]

        p = cells(4, 2, ROWS + 2)
        slope = [(p[i + 2] - p[i]) * (0.5 * SECTION_DT) for i in range(ROWS)]
        top_factor = 1.0 - (c * ROWS).astype(jnp.float32) / depth
        w = cells(2)
        sigma, size, upward = speeds(w, c > 0, c < groups - 1)
        for f in range(4):
            q = w if f == 2 else cells(f)
            flux = line_terms(q, sigma, size, upward)
            for i in range(ROWS):
                value = q[i + 3] + (flux[i + 1] - flux[i])
                rows = pl.ds(base + i * ROWS, ROWS)
                if f == 0:
                    tilt = slope[i] * (top_factor - (i + 0.5) / depth)
                    value = value + east[...] * tilt + turning * zf[1, pl.ds(base + EDGE + i * ROWS, ROWS), :]
                elif f == 1:
                    tilt = slope[i] * (top_factor - (i + 0.5) / depth)
                    value = value + north[...] * tilt - turning * zf[0, pl.ds(base + EDGE + i * ROWS, ROWS), :]
                elif f == 2:
                    warm = zf[3, pl.ds(base + EDGE + i * ROWS, ROWS), :]
                    value = value - slope[i] + warm * (SECTION_DT * BUOYANCY)
                out[f, rows, :] = value
        return carry

    lax.fori_loop(0, groups, upright, 0)

    if near_y:
        pl.semaphore_wait(vouch.at[2], len(near_y))
    each(0, pz, lambda i: tell(vouch.at[4], at_z(i)))
    if far_y:
        for d in (NEAR_Y, ny - NEAR_Y):
            tell(vouch.at[3], at_y(carry(py + d, ny)[0]))

    recv_q[pq] = total_of(recv_a, got_a)

    def to_q(y, z):
        remote(recv_q.at[pq], recv_q.at[pq], send_q, got_q, at_q(y, z)).start()

    def to_columns(columns):
        def visit(z):
            for y in columns:
                to_q(y, z)

        return visit

    if far_y:
        pl.semaphore_wait(vouch.at[3], 2)
    each(0, pz, to_columns([py, *near_y, *far_y]))
    to_columns(near_y + far_y)(pz)

    @pl.when(pz < nz - 1)
    def _():
        pl.semaphore_wait(vouch.at[0], 1)
        x_copies[1].start()

    @pl.when(pz == 0)
    def _():
        pl.semaphore_wait(vouch.at[1], 1)
        x_copies[0].start()

    for copy in x_copies:
        copy.wait_recv()

    edge_rows = jnp.zeros((5, halves, ROWS, LANES), jnp.float32)

    @pl.when(gy == 0)
    def _():
        xt[:, :, pl.ds(0, ROWS), :] = edge_rows

    @pl.when(gy == n_gy - 1)
    def _():
        xt[:, :, pl.ds(ROWS + LANES, ROWS), :] = edge_rows

    gap = jnp.zeros((LANES - 2 * ROWS, LANES), jnp.float32)
    for f in range(2):
        for half in range(halves):
            block = jnp.concatenate(
                [xt[f, half, pl.ds(ROWS + LANES, ROWS), :], gap, xt[f, half, pl.ds(0, ROWS), :]], axis=0
            )
            halo[f, pl.ds(half * LANES, LANES), :] = block.T
    for f in range(2):
        csend[0, f] = halo[f, pl.ds(0, depth, stride=ROWS), :]
        csend[1, f] = halo[f, pl.ds(7, depth, stride=ROWS), :]

    remote(csend.at[0], crecv.at[1], send_h.at[1], got_h.at[1], gx_low).start()
    remote(csend.at[1], crecv.at[0], send_h.at[1], got_h.at[1], gx_high).start()
    step = LANES // ROWS

    def eastward(c, carry):
        half, start = c // 2, lax.rem(c, 2) * ROWS

        def cells(f, first=-3, count=ROWS + 6):
            return [
                xt[f, half, pl.ds(start + (ROWS + first + i), ROWS, stride=step), :] for i in range(count)
            ]

        u = cells(0)
        sigma, size, upward = speeds(u)
        p = cells(4, -1, ROWS + 2)
        for f in range(4):
            q = u if f == 0 else cells(f)
            flux = line_terms(q, sigma, size, upward)
            for i in range(ROWS):
                value = flux[i + 1] - flux[i]
                if f == 0:
                    value = value - (p[i + 2] - p[i]) * (0.5 * SECTION_DT)
                xdiv[f, half, pl.ds(start + i, ROWS, stride=step), :] = value
        return carry

    lax.fori_loop(0, 2 * halves, eastward, 0)

    @pl.when(pz < nz - 1)
    def _():
        pl.semaphore_wait(vouch.at[4], nz - 1 - pz)
        each(pz + 1, nz, to_columns([py, *near_y, *far_y]))

    all_of(yrecv, got_h.at[0])
    for side, at_edge in ((0, gx == 0), (1, gx == n_gx - 1)):

        @pl.when(at_edge)
        def _():
            yrecv[side] = jnp.zeros(yrecv.shape[1:], jnp.float32)

    def row(f, j, g):
        if j < 0:
            return yrecv[0, (j + 3) * 4 + f if f < 4 else 12, pl.ds(g * ROWS, ROWS), :]
        if j >= ROWS:
            return yrecv[1, (j - ROWS) * 4 + f if f < 4 else 12, pl.ds(g * ROWS, ROWS), :]
        return strided(zf, f, EDGE + g * 64 + j)

    def halo_row(f, j, g):
        if j < 0:
            return crecv[0, f, pl.ds(g * ROWS, ROWS), :]
        if j >= ROWS:
            return crecv[1, f, pl.ds(g * ROWS, ROWS), :]
        return strided(halo, f, g * 64 + j)

    def strength(ux, vx, uy, vy):
        cross = uy + vx
        return SMAG_COEF * jnp.sqrt(0.5 * (ux * ux + vy * vy) + 0.25 * (cross * cross) + BACKGROUND)

    def northward(g, carry):
        v = [row(1, j, g) for j in range(-3, ROWS + 3)]
        sigma, size, upward = speeds(v)
        p = [row(4, j, g) for j in range(-1, ROWS + 1)]
        for f in range(4):
            q = v if f == 1 else [row(f, j, g) for j in range(-3, ROWS + 3)]
            flux = line_terms(q, sigma, size, upward)
            for j in range(ROWS):
                value = flux[j + 1] - flux[j]
                if f == 1:
                    value = value - (p[j + 2] - p[j]) * (0.5 * SECTION_DT)
                rows = pl.ds(g * 64 + j, ROWS, stride=ROWS)
                out[f, rows, :] = out[f, rows, :] + value
        return carry

    lax.fori_loop(0, groups, northward, 0)

    def across(inner, outer):
        plus = pltpu.roll(jnp.where(lane == 0, outer, inner), LANES - 1, 1)
        minus = pltpu.roll(jnp.where(lane == LANES - 1, outer, inner), 1, 1)
        return plus - minus

    def eddy_row(j, g):
        u, v = row(0, j, g), row(1, j, g)
        ux, vx = across(u, halo_row(0, j, g)), across(v, halo_row(1, j, g))
        uy, vy = row(0, j + 1, g) - row(0, j - 1, g), row(1, j + 1, g) - row(1, j - 1, g)
        e = strength(ux, vx, uy, vy)
        eddy_y[j + 1, pl.ds(g * ROWS, ROWS), :] = e
        if 0 <= j < ROWS:
            eddy_z[pl.ds(g * 64 + j, ROWS, stride=ROWS), :] = e

    def eddy_side(j, g):
        ux, vx = across(halo_row(0, j, g), row(0, j, g)), across(halo_row(1, j, g), row(1, j, g))
        uy = halo_row(0, j + 1, g) - halo_row(0, j - 1, g)
        vy = halo_row(1, j + 1, g) - halo_row(1, j - 1, g)
        eddy_v[pl.ds(g * 64 + j, ROWS, stride=ROWS), :] = strength(ux, vx, uy, vy)

    def eddies_inside(g, carry):
        for j in range(ROWS):
            eddy_row(j, g)
        for j in range(1, ROWS - 1):
            eddy_side(j, g)
        return carry

    def eddies_rim(g, carry):
        for j in (-1, ROWS):
            eddy_row(j, g)
        for j in (0, ROWS - 1):
            eddy_side(j, g)
        return carry

    lax.fori_loop(0, groups, eddies_inside, 0)
    for half in range(halves):
        eddy_x[half, pl.ds(ROWS, LANES), :] = eddy_z[pl.ds(half * LANES, LANES), :].T

    all_of(crecv, got_h.at[1])
    for side, at_edge in ((0, gx == 0), (1, gx == n_gx - 1)):

        @pl.when(at_edge)
        def _():
            crecv[side] = jnp.zeros(crecv.shape[1:], jnp.float32)

    lax.fori_loop(0, groups, eddies_rim, 0)
    for half in range(halves):
        outer = eddy_v[pl.ds(half * LANES, LANES), :].T
        eddy_x[half, pl.ds(0, ROWS), :] = outer[LANES - ROWS :]
        eddy_x[half, pl.ds(ROWS + LANES, ROWS), :] = outer[:ROWS]

    def mix(e, q, add):
        count = len(e) - 2
        half_sum = [(e[i] + e[i + 1]) * (0.5 * SECTION_DT) for i in range(count + 1)]
        for f in range(4):
            line = q(f)
            flux = [half_sum[i] * (line[i + 1] - line[i]) for i in range(count + 1)]
            for i in range(count):
                add(f, i, flux[i + 1] - flux[i])

    def mix_north(g, carry):
        def add(f, j, value):
            rows = pl.ds(g * 64 + j, ROWS, stride=ROWS)
            out[f, rows, :] = out[f, rows, :] + value

        e = [eddy_y[j, pl.ds(g * ROWS, ROWS), :] for j in range(ROWS + 2)]
        mix(e, lambda f: [row(f, j, g) for j in range(-1, ROWS + 1)], add)
        return carry

    lax.fori_loop(0, groups, mix_north, 0)

    def mix_east(c, carry):
        half, start = c // 2, lax.rem(c, 2) * ROWS

        def line(ref, *lead):
            return [ref[*lead, half, pl.ds(start + (ROWS - 1 + i), ROWS, stride=step), :] for i in range(ROWS + 2)]

        def add(f, i, value):
            rows = pl.ds(start + i, ROWS, stride=step)
            xdiv[f, half, rows, :] = xdiv[f, half, rows, :] + value

        mix(line(eddy_x), lambda f: line(xt, f), add)
        return carry

    lax.fori_loop(0, 2 * halves, mix_east, 0)

    for f in range(4):
        for half in range(halves):
            rows = pl.ds(half * LANES, LANES)
            out[f, rows, :] = out[f, rows, :] + xdiv[f, half].T

    own = total_of(recv_q, got_q)
    scale = SECTION_DT * BUOYANCY / (n_gx * ROWS * n_gy * LANES)
    for g in range(groups):
        mean = jnp.sum(jnp.where(lane == sub + ROWS * g, own * scale, 0.0), axis=1, keepdims=True)
        for j in range(ROWS):
            rows = pl.ds(g * 64 + j, ROWS, stride=ROWS)
            out[2, rows, :] = out[2, rows, :] - mean

    for ref, sem in (
        (others(recv_a), send_a),
        (others(recv_q), send_q),
        (ysend, send_h.at[0]),
        (csend, send_h.at[1]),
    ):
        all_of(ref, sem)
    for copy in x_copies:
        copy.wait_send()


def body(sizes, fields, coriolis, slope_east, slope_north):
    depth = fields.shape[1]
    nx, nl, nc, nh, nz = sizes
    cells = depth * ROWS
    halves = cells // LANES
    f32 = jnp.float32
    hbm = pl.BlockSpec(memory_space=pltpu.HBM)
    dma = pltpu.SemaphoreType.DMA
    arrays = (fields.reshape(5, cells, LANES), coriolis, slope_east, slope_north)
    out = pl.pallas_call(
        functools.partial(kernel, sizes),
        out_shape=jax.ShapeDtypeStruct((4, cells, LANES), f32),
        in_specs=[hbm] * 4,
        out_specs=pl.BlockSpec(memory_space=pltpu.VMEM),
        scratch_shapes=[
            pltpu.VMEM((5, cells + 2 * EDGE, LANES), f32),
            pltpu.VMEM((5, halves, LANES + 2 * ROWS, LANES), f32),
            pltpu.VMEM((2, 13, depth, LANES), f32),
            pltpu.VMEM((2, 13, depth, LANES), f32),
            pltpu.VMEM((2, cells, LANES), f32),
            pltpu.VMEM((2, 2, depth, LANES), f32),
            pltpu.VMEM((2, 2, depth, LANES), f32),
            pltpu.VMEM((ROWS + 2, depth, LANES), f32),
            pltpu.VMEM((cells, LANES), f32),
            pltpu.VMEM((cells, LANES), f32),
            pltpu.VMEM((halves, LANES + 2 * ROWS, LANES), f32),
            pltpu.VMEM((4, halves, LANES, LANES), f32),
            pltpu.VMEM((ROWS, LANES), f32),
            pltpu.VMEM((ROWS, LANES), f32),
            pltpu.SMEM((ROWS,), f32),
            pltpu.VMEM((nx * nc, 1, LANES), f32),
            pltpu.VMEM((nl * nh * nz, 1, LANES), f32),
            dma((6,)), dma, dma, dma, dma, dma((4,)), dma((4,)), pltpu.SemaphoreType.REGULAR((5,)),
        ],
        compiler_params=pltpu.CompilerParams(
            collective_id=0, has_side_effects=True, vmem_limit_bytes=24 * 1024 * 1024
        ),
    )(*(pltpu.with_memory_space_constraint(a, pltpu.HBM) for a in arrays))
    return out.reshape(4, depth, ROWS, LANES)


def solution(mesh):
    return build(mesh, (4, 2, 2, 4, 12))


def build(mesh, sizes):
    finer = Mesh(mesh.devices.reshape(sizes), AXES)
    in_specs = (P(None, None, GX, GY), P(GX), P(GX, GY), P(GX, GY))
    out_specs = P(None, None, GX, GY)
    step = functools.partial(body, sizes)
    return jax.shard_map(step, mesh=finer, in_specs=in_specs, out_specs=out_specs, check_vma=False)
```

```python
import functools

import jax
import jax.numpy as jnp
from jax import lax
from jax.experimental import pallas as pl
from jax.experimental.pallas import tpu as pltpu
from jax.sharding import Mesh
from jax.sharding import PartitionSpec as P

AXES = ("gx_0", "gx_1", "gx_2", "gy_0", "gy_1")
GX = ("gx_0", "gx_1", "gx_2")
GY = ("gy_0", "gy_1")
MESH = pl.DeviceIdType.MESH

WENO_EPS = 1e-06
SECTION_DT = 0.3
SMAG_COEF = 0.06
BACKGROUND = 0.05
BUOYANCY = 0.5

LANES = 128
ROWS = 8
NEAR_Y = 2
CORNER = 16
EDGE = 24


def line_terms(q, sigma, size, upward):
    count = len(q) - 6
    g = [q[i + 1] - q[i] for i in range(count + 5)]
    bend = [g[i + 1] - g[i] for i in range(count + 4)]
    third = [bend[i + 1] - bend[i] for i in range(count + 3)]
    mid, low, high = [], [], []
    for i in range(count + 4):
        before, after, d = g[i], g[i + 1], bend[i]
        a = (d * (4.0 / 3.0)) * d + (before * after + WENO_EPS)
        d2 = d + d
        b = a + after * d2
        c = a - before * d2
        mid.append(a * a)
        low.append(b * b)
        high.append(c * c)
    out = []
    for f in range(count + 1):
        up = upward[f]
        e0 = jnp.where(up, low[f], high[f + 3])
        e1 = jnp.where(up, mid[f + 1], mid[f + 2])
        e2 = jnp.where(up, high[f + 2], low[f + 1])
        curve = jnp.where(up, bend[f + 1], bend[f + 2])
        t0 = jnp.where(up, third[f], third[f + 2])
        u = e0 * 3.0
        v = e2 + e2
        den = e1 * (e2 + u) + u * v
        num = e1 * (u * third[f + 1] + v * t0)
        flux = sigma[f] * ((q[f + 2] + q[f + 3]) - curve * (1.0 / 3.0)) + size[f] * (num / den)
        out.append(flux)
    return out


def speeds(s, keep_first=None, keep_last=None):
    count = len(s) - 6
    sigma = [(s[f + 2] + s[f + 3]) * (-0.25 * SECTION_DT) for f in range(count + 1)]
    if keep_first is not None:
        sigma[0] = jnp.where(keep_first, sigma[0], 0.0)
        sigma[count] = jnp.where(keep_last, sigma[count], 0.0)
    upward = [x < 0.0 for x in sigma]
    size = [jnp.abs(x) * (1.0 / 3.0) for x in sigma]
    return sigma, size, upward


def kernel(
    sizes, fields, coriolis, slope_east, slope_north, out,
    zf, xt, ysend, yrecv, halo, csend, crecv, corner, eddy_y, eddy_z, eddy_v, eddy_x, xdiv, east, north, cor,
    recv_a, recv_q,
    load_sem, send_a, got_a, send_q, got_q, send_h, got_h, vouch,
):
    nx, nl, nc, nh, nz = sizes
    ny = nh * nl
    n_gx, n_gy = nx * nl * nc, nh * nz
    depth = out.shape[1] // ROWS
    groups = depth // ROWS
    px, pl_, pc, ph, pz = (lax.axis_index(a) for a in AXES)
    py = ph * nl + pl_
    main = pl.ds(EDGE, depth * ROWS)
    winds = pl.ds(0, 3)
    loads = [
        pltpu.make_async_copy(fields.at[3], zf.at[3, main], load_sem.at[0]),
        pltpu.make_async_copy(fields.at[winds], zf.at[winds, main], load_sem.at[1]),
        pltpu.make_async_copy(fields.at[4], zf.at[4, main], load_sem.at[2]),
        pltpu.make_async_copy(slope_east, east, load_sem.at[3]),
        pltpu.make_async_copy(slope_north, north, load_sem.at[4]),
        pltpu.make_async_copy(coriolis, cor, load_sem.at[5]),
    ]
    for copy in loads:
        copy.start()

    gx = (px * nl + pl_) * nc + pc
    gy = ph * nz + pz

    def carry(coordinate, size):
        over = coordinate >= size
        return jnp.where(over, coordinate - size, coordinate), over.astype(jnp.int32)

    def step_up(fast, sizes_fast):
        carried, moved = 1, []
        for coordinate, size in zip(fast, sizes_fast, strict=True):
            coordinate, carried = carry(coordinate + carried, size)
            moved.append(coordinate)
        return moved

    def step_down(fast, sizes_fast):
        flipped = [size - 1 - c for c, size in zip(fast, sizes_fast, strict=True)]
        return [size - 1 - c for c, size in zip(step_up(flipped, sizes_fast), sizes_fast, strict=True)]

    def along_gx(step):
        c, l, x = step((pc, pl_, px), (nc, nl, nx))
        return (x, l, c, ph, pz)

    def along_gy(step):
        z, h = step((pz, ph), (nz, nh))
        return (px, pl_, pc, h, z)

    def at_a(i):
        x = lax.div(i, nc)
        return (x, pl_, i - x * nc, ph, pz)

    def at_z(i):
        return (px, pl_, pc, ph, i)

    def at_y(i):
        h = lax.div(i, nl)
        return (px, i - h * nl, pc, h, pz)

    def at_q(y, z):
        return (*at_y(y)[:4], z)

    n_a = nx * nc
    pa, py = px * nc + pc, ph * nl + pl_
    pq = py * nz + pz
    around = [(min(d, ny - d) <= NEAR_Y, carry(py + d, ny)[0]) for d in range(1, ny)]
    near_y, far_y = [y for near, y in around if near], [y for near, y in around if not near]
    gx_low, gx_high = along_gx(step_down), along_gx(step_up)
    gy_low, gy_high = along_gy(step_down), along_gy(step_up)

    barrier = pltpu.get_barrier_semaphore()

    def one(condition):
        return condition.astype(jnp.int32)

    def each(first, last, visit):
        def step(i, unused):
            visit(i)
            return unused

        lax.fori_loop(first, last, step, 0)

    def tell(sem, peer):
        pl.semaphore_signal(sem, inc=1, device_id=peer, device_id_type=MESH)

    by_distance = sorted(range(1, n_a), key=lambda i: -min(i // nc, nx - i // nc))
    together = [at_a(carry(pa + i, n_a)[0]) for i in by_distance] + [at_y(y) for y in near_y] + [gx_low, gx_high]
    for peer in together:
        tell(barrier, peer)
    each(pz + 1, nz, lambda i: tell(barrier, at_z(i)))
    pl.when(pz == 0)(functools.partial(tell, barrier, gy_low))
    expected = len(together) + pz + one(pz == nz - 1)

    lane = lax.broadcasted_iota(jnp.int32, (ROWS, LANES), 1)
    sub = lax.broadcasted_iota(jnp.int32, (ROWS, LANES), 0)

    def strided(ref, f, first):
        return ref[f, pl.ds(first, ROWS, stride=ROWS), :]

    loads[0].wait()
    own = jnp.zeros((ROWS, LANES), jnp.float32)
    for g in range(groups):
        level = strided(zf, 3, EDGE + 64 * g)
        for j in range(1, ROWS):
            level = level + strided(zf, 3, EDGE + 64 * g + j)
        own = own + jnp.where(lane == sub + ROWS * g, jnp.sum(level, axis=1, keepdims=True), 0.0)
    own = jnp.sum(own, axis=0, keepdims=True)
    recv_a[pa] = own

    def remote(src, dst, send, got, peer):
        return pltpu.make_async_remote_copy(
            src_ref=src, dst_ref=dst, send_sem=send, recv_sem=got, device_id=peer, device_id_type=MESH
        )

    def send_row(rows, me, send, got, place):
        return lambda i: remote(rows.at[me], rows.at[me], send, got, place(i)).start()

    def others(rows):
        return rows.at[pl.ds(0, rows.shape[0] - 1)]

    def all_of(ref, sem):
        pltpu.make_async_copy(ref, ref, sem).wait()

    def total_of(rows, got):
        all_of(others(rows), got)
        parts = [rows[i] for i in range(rows.shape[0])]
        while len(parts) > 1:
            parts = [sum(parts[i : i + 2][1:], parts[i]) for i in range(0, len(parts), 2)]
        return parts[0]

    for copy in loads[1:]:
        copy.wait()

    for f in range(5):
        for r in range(3):
            slab = r * 4 + f
            if f == 4:
                if r:
                    continue
                slab = 12
            low_row, high_row = (r, 5 + r) if f < 4 else (0, 7)
            ysend[0, slab] = zf[f, pl.ds(EDGE + low_row, depth, stride=ROWS), :]
            ysend[1, slab] = zf[f, pl.ds(EDGE + high_row, depth, stride=ROWS), :]
        bottom = zf[f, pl.ds(EDGE, ROWS), :]
        top = zf[f, pl.ds(EDGE + (depth - 1) * ROWS, ROWS), :]
        for r in range(3):
            zf[f, pl.ds(r * ROWS, ROWS), :] = bottom
            zf[f, pl.ds(EDGE + (depth + r) * ROWS, ROWS), :] = top
    halves = depth * ROWS // LANES

    for f in range(5):
        for half in range(halves):
            block = zf[f, pl.ds(EDGE + half * LANES, LANES), :]
            xt[f, half, pl.ds(ROWS, LANES), :] = block.T

    pl.semaphore_wait(barrier, expected)
    to_a = send_row(recv_a, pa, send_a, got_a, at_a)
    for i in by_distance:
        to_a(carry(pa + i, n_a)[0])
    for y in near_y:
        tell(vouch.at[2], at_y(y))
    tile_low, tile_high = xt.at[:, :, pl.ds(ROWS, ROWS)], xt.at[:, :, pl.ds(LANES, ROWS)]
    past_low, past_high = xt.at[:, :, pl.ds(0, ROWS)], xt.at[:, :, pl.ds(ROWS + LANES, ROWS)]
    x_copies = [
        remote(tile_low, past_high, send_h.at[2], got_h.at[2], gy_low),
        remote(tile_high, past_low, send_h.at[3], got_h.at[3], gy_high),
    ]
    pl.when(pz == nz - 1)(x_copies[1].start)
    pl.when(pz > 0)(x_copies[0].start)

    def send_rows():
        remote(ysend.at[0], yrecv.at[1], send_h.at[0], got_h.at[0], gx_low).start()
        remote(ysend.at[1], yrecv.at[0], send_h.at[0], got_h.at[0], gx_high).start()

    pl.when(pz < nz // 2)(send_rows)
    pl.when(pz == nz - 1)(functools.partial(tell, vouch.at[1], gy_high))
    pl.when(pz > 0)(functools.partial(tell, vouch.at[0], gy_low))
    turning = jnp.zeros((ROWS, LANES), jnp.float32)
    for j in range(ROWS):
        turning = jnp.where(sub == j, cor[j] * SECTION_DT, turning)

    def upright(c, carry):
        base = c * ROWS * ROWS

        def cells(f, first=0, count=ROWS + 6):
            return [zf[f, pl.ds(base + (first + i) * ROWS, ROWS), :] for i in range(count)]

        p = cells(4, 2, ROWS + 2)
        slope = [(p[i + 2] - p[i]) * (0.5 * SECTION_DT) for i in range(ROWS)]
        top_factor = 1.0 - (c * ROWS).astype(jnp.float32) / depth
        w = cells(2)
        sigma, size, upward = speeds(w, c > 0, c < groups - 1)
        for f in range(4):
            q = w if f == 2 else cells(f)
            flux = line_terms(q, sigma, size, upward)
            for i in range(ROWS):
                value = q[i + 3] + (flux[i + 1] - flux[i])
                rows = pl.ds(base + i * ROWS, ROWS)
                if f == 0:
                    tilt = slope[i] * (top_factor - (i + 0.5) / depth)
                    value = value + east[...] * tilt + turning * zf[1, pl.ds(base + EDGE + i * ROWS, ROWS), :]
                elif f == 1:
                    tilt = slope[i] * (top_factor - (i + 0.5) / depth)
                    value = value + north[...] * tilt - turning * zf[0, pl.ds(base + EDGE + i * ROWS, ROWS), :]
                elif f == 2:
                    warm = zf[3, pl.ds(base + EDGE + i * ROWS, ROWS), :]
                    value = value - slope[i] + warm * (SECTION_DT * BUOYANCY)
                out[f, rows, :] = value
        return carry

    lax.fori_loop(0, groups, upright, 0)

    if near_y:
        pl.semaphore_wait(vouch.at[2], len(near_y))
    close = nz // 2 - 1
    split = jnp.maximum(pz - close, 0)
    each(split, pz, lambda i: tell(vouch.at[4], at_z(i)))
    each(0, split, lambda i: tell(vouch.at[5], at_z(i)))
    last_close = jnp.minimum(pz + close, nz - 1)
    if far_y:
        for d in (NEAR_Y, ny - NEAR_Y):
            tell(vouch.at[3], at_y(carry(py + d, ny)[0]))

    recv_q[pq] = total_of(recv_a, got_a)

    def to_q(y, z):
        remote(recv_q.at[pq], recv_q.at[pq], send_q, got_q, at_q(y, z)).start()

    def to_columns(columns):
        def visit(z):
            for y in columns:
                to_q(y, z)

        return visit

    ahead = jnp.minimum(pz, 2) if far_y else pz
    each(0, ahead, to_columns([py, *near_y]))
    if far_y:
        pl.semaphore_wait(vouch.at[3], 2)
        each(0, ahead, to_columns(far_y))
        each(ahead, pz, to_columns([py, *near_y, *far_y]))
    to_columns(near_y + far_y)(pz)
    pl.when(pz >= nz // 2)(send_rows)

    @pl.when(pz < nz - 1)
    def _():
        pl.semaphore_wait(vouch.at[0], 1)
        x_copies[1].start()
        pl.semaphore_wait(vouch.at[4], last_close - pz)
        each(pz + 1, last_close + 1, to_columns([py, *near_y, *far_y]))

    all_of(yrecv, got_h.at[0])
    for side, at_edge in ((0, gx == 0), (1, gx == n_gx - 1)):

        @pl.when(at_edge)
        def _():
            yrecv[side] = jnp.zeros(yrecv.shape[1:], jnp.float32)

    def row(f, j, g):
        if j < 0:
            return yrecv[0, (j + 3) * 4 + f if f < 4 else 12, pl.ds(g * ROWS, ROWS), :]
        if j >= ROWS:
            return yrecv[1, (j - ROWS) * 4 + f if f < 4 else 12, pl.ds(g * ROWS, ROWS), :]
        return strided(zf, f, EDGE + g * 64 + j)

    def halo_row(f, j, g):
        if 0 <= j < ROWS:
            return strided(halo, f, g * 64 + j)
        return corner[0 if j < 0 else 1, f, pl.ds(g * ROWS, ROWS), :]

    def strength(ux, vx, uy, vy):
        cross = uy + vx
        return SMAG_COEF * jnp.sqrt(0.5 * (ux * ux + vy * vy) + 0.25 * (cross * cross) + BACKGROUND)

    def northward(g, carry):
        v = [row(1, j, g) for j in range(-3, ROWS + 3)]
        sigma, size, upward = speeds(v)
        p = [row(4, j, g) for j in range(-1, ROWS + 1)]
        for f in range(4):
            q = v if f == 1 else [row(f, j, g) for j in range(-3, ROWS + 3)]
            flux = line_terms(q, sigma, size, upward)
            for j in range(ROWS):
                value = flux[j + 1] - flux[j]
                if f == 1:
                    value = value - (p[j + 2] - p[j]) * (0.5 * SECTION_DT)
                rows = pl.ds(g * 64 + j, ROWS, stride=ROWS)
                out[f, rows, :] = out[f, rows, :] + value
        return carry

    lax.fori_loop(0, groups, northward, 0)

    @pl.when(pz == 0)
    def _():
        pl.semaphore_wait(vouch.at[1], 1)
        x_copies[0].start()

    for copy in x_copies:
        copy.wait_recv()

    edge_rows = jnp.zeros((5, halves, ROWS, LANES), jnp.float32)

    @pl.when(gy == 0)
    def _():
        xt[:, :, pl.ds(0, ROWS), :] = edge_rows

    @pl.when(gy == n_gy - 1)
    def _():
        xt[:, :, pl.ds(ROWS + LANES, ROWS), :] = edge_rows

    gap = jnp.zeros((LANES - 2 * ROWS, LANES), jnp.float32)
    for f in range(2):
        for half in range(halves):
            block = jnp.concatenate(
                [xt[f, half, pl.ds(ROWS + LANES, ROWS), :], gap, xt[f, half, pl.ds(0, ROWS), :]], axis=0
            )
            halo[f, pl.ds(half * LANES, LANES), :] = block.T
    place = lax.rem(lane + CORNER // 2, LANES) // CORNER
    for side, j in ((0, 0), (1, ROWS - 1)):
        packed = jnp.zeros((ROWS, LANES), jnp.float32)
        for m in range(2 * groups):
            piece = strided(halo, m // groups, (m % groups) * 64 + j)
            packed = jnp.where(place == m, pltpu.roll(piece, m * CORNER, 1) if m else piece, packed)
        csend[side] = packed

    remote(csend.at[0], crecv.at[1], send_h.at[1], got_h.at[1], gx_low).start()
    remote(csend.at[1], crecv.at[0], send_h.at[1], got_h.at[1], gx_high).start()
    step = LANES // ROWS

    def eastward(c, carry):
        half, start = c // 2, lax.rem(c, 2) * ROWS

        def cells(f, first=-3, count=ROWS + 6):
            return [
                xt[f, half, pl.ds(start + (ROWS + first + i), ROWS, stride=step), :] for i in range(count)
            ]

        u = cells(0)
        sigma, size, upward = speeds(u)
        p = cells(4, -1, ROWS + 2)
        for f in range(4):
            q = u if f == 0 else cells(f)
            flux = line_terms(q, sigma, size, upward)
            for i in range(ROWS):
                value = flux[i + 1] - flux[i]
                if f == 0:
                    value = value - (p[i + 2] - p[i]) * (0.5 * SECTION_DT)
                xdiv[f, half, pl.ds(start + i, ROWS, stride=step), :] = value
        return carry

    lax.fori_loop(0, 2 * halves, eastward, 0)

    def across(inner, outer):
        plus = pltpu.roll(jnp.where(lane == 0, outer, inner), LANES - 1, 1)
        minus = pltpu.roll(jnp.where(lane == LANES - 1, outer, inner), 1, 1)
        return plus - minus

    def eddy_row(j, g):
        u, v = row(0, j, g), row(1, j, g)
        ux, vx = across(u, halo_row(0, j, g)), across(v, halo_row(1, j, g))
        uy, vy = row(0, j + 1, g) - row(0, j - 1, g), row(1, j + 1, g) - row(1, j - 1, g)
        e = strength(ux, vx, uy, vy)
        eddy_y[j + 1, pl.ds(g * ROWS, ROWS), :] = e
        if 0 <= j < ROWS:
            eddy_z[pl.ds(g * 64 + j, ROWS, stride=ROWS), :] = e

    def eddy_side(j, g):
        ux, vx = across(halo_row(0, j, g), row(0, j, g)), across(halo_row(1, j, g), row(1, j, g))
        uy = halo_row(0, j + 1, g) - halo_row(0, j - 1, g)
        vy = halo_row(1, j + 1, g) - halo_row(1, j - 1, g)
        eddy_v[pl.ds(g * 64 + j, ROWS, stride=ROWS), :] = strength(ux, vx, uy, vy)

    def eddies_inside(g, carry):
        for j in range(ROWS):
            eddy_row(j, g)
        for j in range(1, ROWS - 1):
            eddy_side(j, g)
        return carry

    def eddies_rim(g, carry):
        for j in (-1, ROWS):
            eddy_row(j, g)
        for j in (0, ROWS - 1):
            eddy_side(j, g)
        return carry

    lax.fori_loop(0, groups, eddies_inside, 0)
    for half in range(halves):
        eddy_x[half, pl.ds(ROWS, LANES), :] = eddy_z[pl.ds(half * LANES, LANES), :].T

    @pl.when(last_close < nz - 1)
    def _():
        pl.semaphore_wait(vouch.at[5], nz - 1 - last_close)
        each(last_close + 1, nz, to_columns([py, *near_y, *far_y]))

    all_of(crecv, got_h.at[1])
    for side, at_edge in ((0, gx == 0), (1, gx == n_gx - 1)):

        @pl.when(at_edge)
        def _():
            crecv[side] = jnp.zeros(crecv.shape[1:], jnp.float32)

    for side in range(2):
        packed = crecv[side]
        for m in range(2 * groups):
            piece = pltpu.roll(packed, LANES - m * CORNER, 1) if m else packed
            corner[side, m // groups, pl.ds((m % groups) * ROWS, ROWS), :] = piece

    lax.fori_loop(0, groups, eddies_rim, 0)
    for half in range(halves):
        outer = eddy_v[pl.ds(half * LANES, LANES), :].T
        eddy_x[half, pl.ds(0, ROWS), :] = outer[LANES - ROWS :]
        eddy_x[half, pl.ds(ROWS + LANES, ROWS), :] = outer[:ROWS]

    def mix(e, q, add):
        count = len(e) - 2
        half_sum = [(e[i] + e[i + 1]) * (0.5 * SECTION_DT) for i in range(count + 1)]
        for f in range(4):
            line = q(f)
            flux = [half_sum[i] * (line[i + 1] - line[i]) for i in range(count + 1)]
            for i in range(count):
                add(f, i, flux[i + 1] - flux[i])

    def mix_north(g, carry):
        def add(f, j, value):
            rows = pl.ds(g * 64 + j, ROWS, stride=ROWS)
            out[f, rows, :] = out[f, rows, :] + value

        e = [eddy_y[j, pl.ds(g * ROWS, ROWS), :] for j in range(ROWS + 2)]
        mix(e, lambda f: [row(f, j, g) for j in range(-1, ROWS + 1)], add)
        return carry

    lax.fori_loop(0, groups, mix_north, 0)

    def mix_east(c, carry):
        half, start = c // 2, lax.rem(c, 2) * ROWS

        def line(ref, *lead):
            return [ref[*lead, half, pl.ds(start + (ROWS - 1 + i), ROWS, stride=step), :] for i in range(ROWS + 2)]

        def add(f, i, value):
            rows = pl.ds(start + i, ROWS, stride=step)
            xdiv[f, half, rows, :] = xdiv[f, half, rows, :] + value

        mix(line(eddy_x), lambda f: line(xt, f), add)
        return carry

    lax.fori_loop(0, 2 * halves, mix_east, 0)

    for f in range(4):
        for half in range(halves):
            rows = pl.ds(half * LANES, LANES)
            out[f, rows, :] = out[f, rows, :] + xdiv[f, half].T

    own = total_of(recv_q, got_q)
    scale = SECTION_DT * BUOYANCY / (n_gx * ROWS * n_gy * LANES)
    for g in range(groups):
        mean = jnp.sum(jnp.where(lane == sub + ROWS * g, own * scale, 0.0), axis=1, keepdims=True)
        for j in range(ROWS):
            rows = pl.ds(g * 64 + j, ROWS, stride=ROWS)
            out[2, rows, :] = out[2, rows, :] - mean

    for ref, sem in (
        (others(recv_a), send_a),
        (others(recv_q), send_q),
        (ysend, send_h.at[0]),
        (csend, send_h.at[1]),
    ):
        all_of(ref, sem)
    for copy in x_copies:
        copy.wait_send()


def body(sizes, fields, coriolis, slope_east, slope_north):
    depth = fields.shape[1]
    nx, nl, nc, nh, nz = sizes
    cells = depth * ROWS
    halves = cells // LANES
    f32 = jnp.float32
    hbm = pl.BlockSpec(memory_space=pltpu.HBM)
    dma = pltpu.SemaphoreType.DMA
    arrays = (fields.reshape(5, cells, LANES), coriolis, slope_east, slope_north)
    out = pl.pallas_call(
        functools.partial(kernel, sizes),
        out_shape=jax.ShapeDtypeStruct((4, cells, LANES), f32),
        in_specs=[hbm] * 4,
        out_specs=pl.BlockSpec(memory_space=pltpu.VMEM),
        scratch_shapes=[
            pltpu.VMEM((5, cells + 2 * EDGE, LANES), f32),
            pltpu.VMEM((5, halves, LANES + 2 * ROWS, LANES), f32),
            pltpu.VMEM((2, 13, depth, LANES), f32),
            pltpu.VMEM((2, 13, depth, LANES), f32),
            pltpu.VMEM((2, cells, LANES), f32),
            pltpu.VMEM((2, ROWS, LANES), f32),
            pltpu.VMEM((2, ROWS, LANES), f32),
            pltpu.VMEM((2, 2, depth, LANES), f32),
            pltpu.VMEM((ROWS + 2, depth, LANES), f32),
            pltpu.VMEM((cells, LANES), f32),
            pltpu.VMEM((cells, LANES), f32),
            pltpu.VMEM((halves, LANES + 2 * ROWS, LANES), f32),
            pltpu.VMEM((4, halves, LANES, LANES), f32),
            pltpu.VMEM((ROWS, LANES), f32),
            pltpu.VMEM((ROWS, LANES), f32),
            pltpu.SMEM((ROWS,), f32),
            pltpu.VMEM((nx * nc, 1, LANES), f32),
            pltpu.VMEM((nl * nh * nz, 1, LANES), f32),
            dma((6,)), dma, dma, dma, dma, dma((4,)), dma((4,)), pltpu.SemaphoreType.REGULAR((6,)),
        ],
        compiler_params=pltpu.CompilerParams(
            collective_id=0, has_side_effects=True, vmem_limit_bytes=24 * 1024 * 1024
        ),
    )(*(pltpu.with_memory_space_constraint(a, pltpu.HBM) for a in arrays))
    return out.reshape(4, depth, ROWS, LANES)


def solution(mesh):
    return build(mesh, (4, 2, 2, 4, 12))


def build(mesh, sizes):
    finer = Mesh(mesh.devices.reshape(sizes), AXES)
    in_specs = (P(None, None, GX, GY), P(GX), P(GX, GY), P(GX, GY))
    out_specs = P(None, None, GX, GY)
    step = functools.partial(body, sizes)
    return jax.shard_map(step, mesh=finer, in_specs=in_specs, out_specs=out_specs, check_vma=False)
```

```python
import functools

import jax
import jax.numpy as jnp
from jax import lax
from jax.experimental import pallas as pl
from jax.experimental.pallas import tpu as pltpu
from jax.sharding import Mesh
from jax.sharding import PartitionSpec as P

AXES = ("gx_0", "gx_1", "gx_2", "gy_0", "gy_1")
GX = ("gx_0", "gx_1", "gx_2")
GY = ("gy_0", "gy_1")
MESH = pl.DeviceIdType.MESH

WENO_EPS = 1e-06
SECTION_DT = 0.3
SMAG_COEF = 0.06
BACKGROUND = 0.05
BUOYANCY = 0.5

LANES = 128
ROWS = 8
NEAR_Y = 2
CORNER = 16
EDGE = 24


def line_terms(q, sigma, size, upward):
    count = len(q) - 6
    g = [q[i + 1] - q[i] for i in range(count + 5)]
    bend = [g[i + 1] - g[i] for i in range(count + 4)]
    third = [bend[i + 1] - bend[i] for i in range(count + 3)]
    mid, low, high = [], [], []
    for i in range(count + 4):
        before, after, d = g[i], g[i + 1], bend[i]
        a = (d * (4.0 / 3.0)) * d + (before * after + WENO_EPS)
        d2 = d + d
        b = a + after * d2
        c = a - before * d2
        mid.append(a * a)
        low.append(b * b)
        high.append(c * c)
    out = []
    for f in range(count + 1):
        up = upward[f]
        e0 = jnp.where(up, low[f], high[f + 3])
        e1 = jnp.where(up, mid[f + 1], mid[f + 2])
        e2 = jnp.where(up, high[f + 2], low[f + 1])
        curve = jnp.where(up, bend[f + 1], bend[f + 2])
        t0 = jnp.where(up, third[f], third[f + 2])
        u = e0 * 3.0
        v = e2 + e2
        den = e1 * (e2 + u) + u * v
        num = e1 * (u * third[f + 1] + v * t0)
        flux = sigma[f] * ((q[f + 2] + q[f + 3]) - curve * (1.0 / 3.0)) + size[f] * (num / den)
        out.append(flux)
    return out


def speeds(s, keep_first=None, keep_last=None):
    count = len(s) - 6
    sigma = [(s[f + 2] + s[f + 3]) * (-0.25 * SECTION_DT) for f in range(count + 1)]
    if keep_first is not None:
        sigma[0] = jnp.where(keep_first, sigma[0], 0.0)
        sigma[count] = jnp.where(keep_last, sigma[count], 0.0)
    upward = [x < 0.0 for x in sigma]
    size = [jnp.abs(x) * (1.0 / 3.0) for x in sigma]
    return sigma, size, upward


def kernel(
    sizes, fields, coriolis, slope_east, slope_north, out,
    zf, xt, ysend, yrecv, halo, csend, crecv, corner, eddy_y, eddy_z, eddy_v, eddy_x, xdiv, east, north, cor,
    recv_a, recv_q,
    load_sem, send_a, got_a, send_q, got_q, send_h, got_h, vouch,
):
    nx, nl, nc, nh, nz = sizes
    ny = nh * nl
    n_gx, n_gy = nx * nl * nc, nh * nz
    depth = out.shape[1] // ROWS
    groups = depth // ROWS
    px, pl_, pc, ph, pz = (lax.axis_index(a) for a in AXES)
    py = ph * nl + pl_
    main = pl.ds(EDGE, depth * ROWS)
    winds = pl.ds(0, 3)
    loads = [
        pltpu.make_async_copy(fields.at[3], zf.at[3, main], load_sem.at[0]),
        pltpu.make_async_copy(fields.at[winds], zf.at[winds, main], load_sem.at[1]),
        pltpu.make_async_copy(fields.at[4], zf.at[4, main], load_sem.at[1]),
        pltpu.make_async_copy(slope_east, east, load_sem.at[2]),
        pltpu.make_async_copy(slope_north, north, load_sem.at[3]),
        pltpu.make_async_copy(coriolis, cor, load_sem.at[4]),
    ]
    for copy in loads:
        copy.start()

    gx = (px * nl + pl_) * nc + pc
    gy = ph * nz + pz

    def carry(coordinate, size):
        over = coordinate >= size
        return jnp.where(over, coordinate - size, coordinate), over.astype(jnp.int32)

    def step_up(fast, sizes_fast):
        carried, moved = 1, []
        for coordinate, size in zip(fast, sizes_fast, strict=True):
            coordinate, carried = carry(coordinate + carried, size)
            moved.append(coordinate)
        return moved

    def step_down(fast, sizes_fast):
        flipped = [size - 1 - c for c, size in zip(fast, sizes_fast, strict=True)]
        return [size - 1 - c for c, size in zip(step_up(flipped, sizes_fast), sizes_fast, strict=True)]

    def along_gx(step):
        c, l, x = step((pc, pl_, px), (nc, nl, nx))
        return (x, l, c, ph, pz)

    def along_gy(step):
        z, h = step((pz, ph), (nz, nh))
        return (px, pl_, pc, h, z)

    def at_a(i):
        x = lax.div(i, nc)
        return (x, pl_, i - x * nc, ph, pz)

    def at_z(i):
        return (px, pl_, pc, ph, i)

    def at_y(i):
        h = lax.div(i, nl)
        return (px, i - h * nl, pc, h, pz)

    def at_q(y, z):
        return (*at_y(y)[:4], z)

    n_a = nx * nc
    pa, py = px * nc + pc, ph * nl + pl_
    pq = py * nz + pz
    around = [(min(d, ny - d) <= NEAR_Y, carry(py + d, ny)[0]) for d in range(1, ny)]
    near_y, far_y = [y for near, y in around if near], [y for near, y in around if not near]
    gx_low, gx_high = along_gx(step_down), along_gx(step_up)
    gy_low, gy_high = along_gy(step_down), along_gy(step_up)

    barrier = pltpu.get_barrier_semaphore()

    def one(condition):
        return condition.astype(jnp.int32)

    def each(first, last, visit):
        def step(i, unused):
            visit(i)
            return unused

        lax.fori_loop(first, last, step, 0)

    def tell(sem, peer):
        pl.semaphore_signal(sem, inc=1, device_id=peer, device_id_type=MESH)

    by_distance = sorted(range(1, n_a), key=lambda i: -min(i // nc, nx - i // nc))
    far_first = sorted(range(1, ny), key=lambda d: (-min(d, ny - d), -d))
    steps = [d for d in far_first if min(d, ny - d) <= NEAR_Y]
    together = [at_y(carry(py + d, ny)[0]) for d in steps]
    together += [at_a(carry(pa + i, n_a)[0]) for i in by_distance] + [gx_low, gx_high]
    for peer in together:
        tell(barrier, peer)
    each(pz + 1, nz, lambda i: tell(barrier, at_z(i)))
    pl.when(pz == 0)(functools.partial(tell, barrier, gy_low))
    expected = len(together) + pz + one(pz == nz - 1)

    lane = lax.broadcasted_iota(jnp.int32, (ROWS, LANES), 1)
    sub = lax.broadcasted_iota(jnp.int32, (ROWS, LANES), 0)

    def strided(ref, f, first):
        return ref[f, pl.ds(first, ROWS, stride=ROWS), :]

    loads[0].wait()
    own = jnp.zeros((ROWS, LANES), jnp.float32)
    for g in range(groups):
        level = strided(zf, 3, EDGE + 64 * g)
        for j in range(1, ROWS):
            level = level + strided(zf, 3, EDGE + 64 * g + j)
        own = own + jnp.where(lane == sub + ROWS * g, jnp.sum(level, axis=1, keepdims=True), 0.0)
    own = jnp.sum(own, axis=0, keepdims=True)
    recv_a[pa] = own

    def remote(src, dst, send, got, peer):
        return pltpu.make_async_remote_copy(
            src_ref=src, dst_ref=dst, send_sem=send, recv_sem=got, device_id=peer, device_id_type=MESH
        )

    def send_row(rows, me, send, got, place):
        return lambda i: remote(rows.at[me], rows.at[me], send, got, place(i)).start()

    def others(rows):
        return rows.at[pl.ds(0, rows.shape[0] - 1)]

    def all_of(ref, sem):
        pltpu.make_async_copy(ref, ref, sem).wait()

    def total_of(rows, got):
        all_of(others(rows), got)
        parts = [rows[i] for i in range(rows.shape[0])]
        while len(parts) > 1:
            parts = [sum(parts[i : i + 2][1:], parts[i]) for i in range(0, len(parts), 2)]
        return parts[0]

    all_of(zf.at[pl.ds(0, 4), main], load_sem.at[1])
    for copy in loads[3:]:
        copy.wait()

    for f in range(5):
        for r in range(3):
            slab = r * 4 + f
            if f == 4:
                if r:
                    continue
                slab = 12
            low_row, high_row = (r, 5 + r) if f < 4 else (0, 7)
            ysend[0, slab] = zf[f, pl.ds(EDGE + low_row, depth, stride=ROWS), :]
            ysend[1, slab] = zf[f, pl.ds(EDGE + high_row, depth, stride=ROWS), :]
        bottom = zf[f, pl.ds(EDGE, ROWS), :]
        top = zf[f, pl.ds(EDGE + (depth - 1) * ROWS, ROWS), :]
        for r in range(3):
            zf[f, pl.ds(r * ROWS, ROWS), :] = bottom
            zf[f, pl.ds(EDGE + (depth + r) * ROWS, ROWS), :] = top
    halves = depth * ROWS // LANES

    for f in range(5):
        for half in range(halves):
            block = zf[f, pl.ds(EDGE + half * LANES, LANES), :]
            xt[f, half, pl.ds(ROWS, LANES), :] = block.T

    pl.semaphore_wait(barrier, expected)
    to_a = send_row(recv_a, pa, send_a, got_a, at_a)
    for i in by_distance:
        to_a(carry(pa + i, n_a)[0])
    for y in near_y:
        tell(vouch.at[2], at_y(y))
    tile_low, tile_high = xt.at[:, :, pl.ds(ROWS, ROWS)], xt.at[:, :, pl.ds(LANES, ROWS)]
    past_low, past_high = xt.at[:, :, pl.ds(0, ROWS)], xt.at[:, :, pl.ds(ROWS + LANES, ROWS)]
    x_copies = [
        remote(tile_low, past_high, send_h.at[2], got_h.at[2], gy_low),
        remote(tile_high, past_low, send_h.at[3], got_h.at[3], gy_high),
    ]
    pl.when(pz == nz - 1)(x_copies[1].start)
    pl.when(pz > 0)(x_copies[0].start)

    def send_rows():
        remote(ysend.at[0], yrecv.at[1], send_h.at[0], got_h.at[0], gx_low).start()
        remote(ysend.at[1], yrecv.at[0], send_h.at[0], got_h.at[0], gx_high).start()

    pl.when(pz < nz // 2)(send_rows)
    pl.when(pz == nz - 1)(functools.partial(tell, vouch.at[1], gy_high))
    pl.when(pz > 0)(functools.partial(tell, vouch.at[0], gy_low))
    turning = jnp.zeros((ROWS, LANES), jnp.float32)
    for j in range(ROWS):
        turning = jnp.where(sub == j, cor[j] * SECTION_DT, turning)

    def upright(c, carry):
        base = c * ROWS * ROWS

        def cells(f, first=0, count=ROWS + 6):
            return [zf[f, pl.ds(base + (first + i) * ROWS, ROWS), :] for i in range(count)]

        p = cells(4, 2, ROWS + 2)
        slope = [(p[i + 2] - p[i]) * (0.5 * SECTION_DT) for i in range(ROWS)]
        top_factor = 1.0 - (c * ROWS).astype(jnp.float32) / depth
        w = cells(2)
        sigma, size, upward = speeds(w, c > 0, c < groups - 1)
        for f in range(4):
            q = w if f == 2 else cells(f)
            flux = line_terms(q, sigma, size, upward)
            for i in range(ROWS):
                value = q[i + 3] + (flux[i + 1] - flux[i])
                rows = pl.ds(base + i * ROWS, ROWS)
                if f == 0:
                    tilt = slope[i] * (top_factor - (i + 0.5) / depth)
                    value = value + east[...] * tilt + turning * zf[1, pl.ds(base + EDGE + i * ROWS, ROWS), :]
                elif f == 1:
                    tilt = slope[i] * (top_factor - (i + 0.5) / depth)
                    value = value + north[...] * tilt - turning * zf[0, pl.ds(base + EDGE + i * ROWS, ROWS), :]
                elif f == 2:
                    warm = zf[3, pl.ds(base + EDGE + i * ROWS, ROWS), :]
                    value = value - slope[i] + warm * (SECTION_DT * BUOYANCY)
                out[f, rows, :] = value
        return carry

    lax.fori_loop(0, groups, upright, 0)

    if near_y:
        pl.semaphore_wait(vouch.at[2], len(near_y))
    close = nz // 2 - 1
    split = jnp.maximum(pz - close, 0)
    each(split, pz, lambda i: tell(vouch.at[4], at_z(i)))
    each(0, split, lambda i: tell(vouch.at[5], at_z(i)))
    last_close = jnp.minimum(pz + close, nz - 1)
    if far_y:
        for d in (NEAR_Y, ny - NEAR_Y):
            tell(vouch.at[3], at_y(carry(py + d, ny)[0]))

    recv_q[pq] = total_of(recv_a, got_a)

    def to_q(y, z):
        remote(recv_q.at[pq], recv_q.at[pq], send_q, got_q, at_q(y, z)).start()

    def to_columns(columns):
        def visit(z):
            for y in columns:
                to_q(y, z)

        return visit

    ahead = jnp.minimum(pz, 2) if far_y else pz
    each(0, ahead, to_columns([py, *near_y]))
    if far_y:
        pl.semaphore_wait(vouch.at[3], 2)
        each(0, ahead, to_columns(far_y))
        each(ahead, pz, to_columns([py, *near_y, *far_y]))
    to_columns(near_y + far_y)(pz)
    pl.when(pz >= nz // 2)(send_rows)

    @pl.when(pz < nz - 1)
    def _():
        pl.semaphore_wait(vouch.at[0], 1)
        x_copies[1].start()
        pl.semaphore_wait(vouch.at[4], last_close - pz)
        each(pz + 1, last_close + 1, to_columns([py, *near_y, *far_y]))

    all_of(yrecv, got_h.at[0])
    for side, at_edge in ((0, gx == 0), (1, gx == n_gx - 1)):

        @pl.when(at_edge)
        def _():
            yrecv[side] = jnp.zeros(yrecv.shape[1:], jnp.float32)

    def row(f, j, g):
        if j < 0:
            return yrecv[0, (j + 3) * 4 + f if f < 4 else 12, pl.ds(g * ROWS, ROWS), :]
        if j >= ROWS:
            return yrecv[1, (j - ROWS) * 4 + f if f < 4 else 12, pl.ds(g * ROWS, ROWS), :]
        return strided(zf, f, EDGE + g * 64 + j)

    def halo_row(f, j, g):
        if 0 <= j < ROWS:
            return strided(halo, f, g * 64 + j)
        return corner[0 if j < 0 else 1, f, pl.ds(g * ROWS, ROWS), :]

    def strength(ux, vx, uy, vy):
        cross = uy + vx
        return SMAG_COEF * jnp.sqrt(0.5 * (ux * ux + vy * vy) + 0.25 * (cross * cross) + BACKGROUND)

    def northward(g, carry):
        v = [row(1, j, g) for j in range(-3, ROWS + 3)]
        sigma, size, upward = speeds(v)
        p = [row(4, j, g) for j in range(-1, ROWS + 1)]
        for f in range(4):
            q = v if f == 1 else [row(f, j, g) for j in range(-3, ROWS + 3)]
            flux = line_terms(q, sigma, size, upward)
            for j in range(ROWS):
                value = flux[j + 1] - flux[j]
                if f == 1:
                    value = value - (p[j + 2] - p[j]) * (0.5 * SECTION_DT)
                rows = pl.ds(g * 64 + j, ROWS, stride=ROWS)
                out[f, rows, :] = out[f, rows, :] + value
        return carry

    lax.fori_loop(0, groups, northward, 0)

    @pl.when(pz == 0)
    def _():
        pl.semaphore_wait(vouch.at[1], 1)
        x_copies[0].start()

    for copy in x_copies:
        copy.wait_recv()

    edge_rows = jnp.zeros((5, halves, ROWS, LANES), jnp.float32)

    @pl.when(gy == 0)
    def _():
        xt[:, :, pl.ds(0, ROWS), :] = edge_rows

    @pl.when(gy == n_gy - 1)
    def _():
        xt[:, :, pl.ds(ROWS + LANES, ROWS), :] = edge_rows

    gap = jnp.zeros((LANES - 2 * ROWS, LANES), jnp.float32)
    for f in range(2):
        for half in range(halves):
            block = jnp.concatenate(
                [xt[f, half, pl.ds(ROWS + LANES, ROWS), :], gap, xt[f, half, pl.ds(0, ROWS), :]], axis=0
            )
            halo[f, pl.ds(half * LANES, LANES), :] = block.T
    place = lax.rem(lane + CORNER // 2, LANES) // CORNER
    for side, j in ((0, 0), (1, ROWS - 1)):
        packed = jnp.zeros((ROWS, LANES), jnp.float32)
        for m in range(2 * groups):
            piece = strided(halo, m // groups, (m % groups) * 64 + j)
            packed = jnp.where(place == m, pltpu.roll(piece, m * CORNER, 1) if m else piece, packed)
        csend[side] = packed

    remote(csend.at[0], crecv.at[1], send_h.at[1], got_h.at[1], gx_low).start()
    remote(csend.at[1], crecv.at[0], send_h.at[1], got_h.at[1], gx_high).start()
    step = LANES // ROWS

    def eastward(c, carry):
        half, start = c // 2, lax.rem(c, 2) * ROWS

        def cells(f, first=-3, count=ROWS + 6):
            return [
                xt[f, half, pl.ds(start + (ROWS + first + i), ROWS, stride=step), :] for i in range(count)
            ]

        u = cells(0)
        sigma, size, upward = speeds(u)
        p = cells(4, -1, ROWS + 2)
        for f in range(4):
            q = u if f == 0 else cells(f)
            flux = line_terms(q, sigma, size, upward)
            for i in range(ROWS):
                value = flux[i + 1] - flux[i]
                if f == 0:
                    value = value - (p[i + 2] - p[i]) * (0.5 * SECTION_DT)
                xdiv[f, half, pl.ds(start + i, ROWS, stride=step), :] = value
        return carry

    lax.fori_loop(0, 2 * halves, eastward, 0)

    def across(inner, outer):
        plus = pltpu.roll(jnp.where(lane == 0, outer, inner), LANES - 1, 1)
        minus = pltpu.roll(jnp.where(lane == LANES - 1, outer, inner), 1, 1)
        return plus - minus

    def eddy_row(j, g):
        u, v = row(0, j, g), row(1, j, g)
        ux, vx = across(u, halo_row(0, j, g)), across(v, halo_row(1, j, g))
        uy, vy = row(0, j + 1, g) - row(0, j - 1, g), row(1, j + 1, g) - row(1, j - 1, g)
        e = strength(ux, vx, uy, vy)
        eddy_y[j + 1, pl.ds(g * ROWS, ROWS), :] = e
        if 0 <= j < ROWS:
            eddy_z[pl.ds(g * 64 + j, ROWS, stride=ROWS), :] = e

    def eddy_side(j, g):
        ux, vx = across(halo_row(0, j, g), row(0, j, g)), across(halo_row(1, j, g), row(1, j, g))
        uy = halo_row(0, j + 1, g) - halo_row(0, j - 1, g)
        vy = halo_row(1, j + 1, g) - halo_row(1, j - 1, g)
        eddy_v[pl.ds(g * 64 + j, ROWS, stride=ROWS), :] = strength(ux, vx, uy, vy)

    def eddies_inside(g, carry):
        for j in range(ROWS):
            eddy_row(j, g)
        for j in range(1, ROWS - 1):
            eddy_side(j, g)
        return carry

    def eddies_rim(g, carry):
        for j in (-1, ROWS):
            eddy_row(j, g)
        for j in (0, ROWS - 1):
            eddy_side(j, g)
        return carry

    lax.fori_loop(0, groups, eddies_inside, 0)
    for half in range(halves):
        eddy_x[half, pl.ds(ROWS, LANES), :] = eddy_z[pl.ds(half * LANES, LANES), :].T

    @pl.when(last_close < nz - 1)
    def _():
        pl.semaphore_wait(vouch.at[5], nz - 1 - last_close)
        each(last_close + 1, nz, to_columns([py, *near_y, *far_y]))

    all_of(crecv, got_h.at[1])
    for side, at_edge in ((0, gx == 0), (1, gx == n_gx - 1)):

        @pl.when(at_edge)
        def _():
            crecv[side] = jnp.zeros(crecv.shape[1:], jnp.float32)

    for side in range(2):
        packed = crecv[side]
        for m in range(2 * groups):
            piece = pltpu.roll(packed, LANES - m * CORNER, 1) if m else packed
            corner[side, m // groups, pl.ds((m % groups) * ROWS, ROWS), :] = piece

    lax.fori_loop(0, groups, eddies_rim, 0)
    for half in range(halves):
        outer = eddy_v[pl.ds(half * LANES, LANES), :].T
        eddy_x[half, pl.ds(0, ROWS), :] = outer[LANES - ROWS :]
        eddy_x[half, pl.ds(ROWS + LANES, ROWS), :] = outer[:ROWS]

    def mix(e, q, add):
        count = len(e) - 2
        half_sum = [(e[i] + e[i + 1]) * (0.5 * SECTION_DT) for i in range(count + 1)]
        for f in range(4):
            line = q(f)
            flux = [half_sum[i] * (line[i + 1] - line[i]) for i in range(count + 1)]
            for i in range(count):
                add(f, i, flux[i + 1] - flux[i])

    def mix_north(g, carry):
        def add(f, j, value):
            rows = pl.ds(g * 64 + j, ROWS, stride=ROWS)
            out[f, rows, :] = out[f, rows, :] + value

        e = [eddy_y[j, pl.ds(g * ROWS, ROWS), :] for j in range(ROWS + 2)]
        mix(e, lambda f: [row(f, j, g) for j in range(-1, ROWS + 1)], add)
        return carry

    lax.fori_loop(0, groups, mix_north, 0)

    def mix_east(c, carry):
        half, start = c // 2, lax.rem(c, 2) * ROWS

        def line(ref, *lead):
            return [ref[*lead, half, pl.ds(start + (ROWS - 1 + i), ROWS, stride=step), :] for i in range(ROWS + 2)]

        def add(f, i, value):
            rows = pl.ds(start + i, ROWS, stride=step)
            xdiv[f, half, rows, :] = xdiv[f, half, rows, :] + value

        mix(line(eddy_x), lambda f: line(xt, f), add)
        return carry

    lax.fori_loop(0, 2 * halves, mix_east, 0)

    for f in range(4):
        for half in range(halves):
            rows = pl.ds(half * LANES, LANES)
            out[f, rows, :] = out[f, rows, :] + xdiv[f, half].T

    own = total_of(recv_q, got_q)
    scale = SECTION_DT * BUOYANCY / (n_gx * ROWS * n_gy * LANES)
    for g in range(groups):
        mean = jnp.sum(jnp.where(lane == sub + ROWS * g, own * scale, 0.0), axis=1, keepdims=True)
        for j in range(ROWS):
            rows = pl.ds(g * 64 + j, ROWS, stride=ROWS)
            out[2, rows, :] = out[2, rows, :] - mean

    for ref, sem in (
        (others(recv_a), send_a),
        (others(recv_q), send_q),
        (ysend, send_h.at[0]),
        (csend, send_h.at[1]),
    ):
        all_of(ref, sem)
    for copy in x_copies:
        copy.wait_send()


def body(sizes, fields, coriolis, slope_east, slope_north):
    depth = fields.shape[1]
    nx, nl, nc, nh, nz = sizes
    cells = depth * ROWS
    halves = cells // LANES
    f32 = jnp.float32
    hbm = pl.BlockSpec(memory_space=pltpu.HBM)
    dma = pltpu.SemaphoreType.DMA
    arrays = (fields.reshape(5, cells, LANES), coriolis, slope_east, slope_north)
    out = pl.pallas_call(
        functools.partial(kernel, sizes),
        out_shape=jax.ShapeDtypeStruct((4, cells, LANES), f32),
        in_specs=[hbm] * 4,
        out_specs=pl.BlockSpec(memory_space=pltpu.VMEM),
        scratch_shapes=[
            pltpu.VMEM((5, cells + 2 * EDGE, LANES), f32),
            pltpu.VMEM((5, halves, LANES + 2 * ROWS, LANES), f32),
            pltpu.VMEM((2, 13, depth, LANES), f32),
            pltpu.VMEM((2, 13, depth, LANES), f32),
            pltpu.VMEM((2, cells, LANES), f32),
            pltpu.VMEM((2, ROWS, LANES), f32),
            pltpu.VMEM((2, ROWS, LANES), f32),
            pltpu.VMEM((2, 2, depth, LANES), f32),
            pltpu.VMEM((ROWS + 2, depth, LANES), f32),
            pltpu.VMEM((cells, LANES), f32),
            pltpu.VMEM((cells, LANES), f32),
            pltpu.VMEM((halves, LANES + 2 * ROWS, LANES), f32),
            pltpu.VMEM((4, halves, LANES, LANES), f32),
            pltpu.VMEM((ROWS, LANES), f32),
            pltpu.VMEM((ROWS, LANES), f32),
            pltpu.SMEM((ROWS,), f32),
            pltpu.VMEM((nx * nc, 1, LANES), f32),
            pltpu.VMEM((nl * nh * nz, 1, LANES), f32),
            dma((5,)), dma, dma, dma, dma, dma((4,)), dma((4,)), pltpu.SemaphoreType.REGULAR((6,)),
        ],
        compiler_params=pltpu.CompilerParams(
            collective_id=0, has_side_effects=True, vmem_limit_bytes=24 * 1024 * 1024
        ),
    )(*(pltpu.with_memory_space_constraint(a, pltpu.HBM) for a in arrays))
    return out.reshape(4, depth, ROWS, LANES)


def solution(mesh):
    return build(mesh, (4, 2, 2, 4, 12))


def build(mesh, sizes):
    finer = Mesh(mesh.devices.reshape(sizes), AXES)
    in_specs = (P(None, None, GX, GY), P(GX), P(GX, GY), P(GX, GY))
    out_specs = P(None, None, GX, GY)
    step = functools.partial(body, sizes)
    return jax.shard_map(step, mesh=finer, in_specs=in_specs, out_specs=out_specs, check_vma=False)
```
